128 devices in a mesh: dp: 128 (over x, y, z, core).
Axes of the slice: x: 4, y: 4, z: 4, core: 2. Of those that a mesh axis runs over, the one named last changes fastest.
Arguments:
- features: bfloat16 [131072, 3136], P('dp'), may hold values from -6 to 6
- w_one: bfloat16 [512, 3136], replicated, may hold values from -0.109375 to 0.109375
- b_one: float32 [512], replicated, may hold values from -3 to 3
- w_two: bfloat16 [512, 918], replicated, may hold values from -0.25 to 0.25
- b_two: float32 [918], replicated, may hold values from -112 to 112
- action: int32 [131072], P('dp'), may hold values from 0 to 17
- target_probs: float32 [131072, 18, 51], P('dp'), may hold values from 0 to 1, as said below
- next_action: int32 [131072], P('dp'), may hold values from 0 to 17
- lower_idx: int32 [131072, 51], P('dp'), may hold values from 0 to 49
- upper_frac: float32 [131072, 51], P('dp'), may hold values from 0 to 1
- is_weight: float32 [131072], P('dp'), may hold values from 0.1 to 1
Outputs:
- grad_w1: float32 [512, 3136], replicated
- grad_b1: float32 [512], replicated
- grad_w2: float32 [512, 918], replicated
- grad_b2: float32 [918], replicated
- mean_loss: float32 [], replicated
- priorities: float32 [131072], P('dp')
The draws below stay inside these ranges and needn't reach their ends.
Inputs may be any that keep to these rules, and one draw needn't show every extreme that they name: Each target_probs[i, a] is a distribution over the atoms: positive entries that sum to one.
All inputs are finite; a program needn't handle non-finite values.
Results may differ from the reference program's by a relative error of at most 0.005.
Values sent between devices are 32-bit elements; how exact they have to be, the bound alone decides.
A program may use at most 128 MiB of HBM per device.

```python
import math
import jax
import jax.numpy as jnp
from jax import lax

FEAT = 3136
HID = 512
ACTIONS = 18
ATOMS = 51
ROWS = 1024
TOTAL = 131072
N_DP = 128


def draw_b_two(key, part):
    key_noise, key_shift, key_order = jax.random.split(key, 3)
    return jnp.clip(0.5 * jax.random.normal(key_noise, (ACTIONS * ATOMS,), jnp.float32), -2.0, 2.0)


def draw_target_probs(key, part):
    key_main, key_scale = jax.random.split(key, 2)
    scores = 1.5 * jax.random.normal(key_main, (TOTAL, ACTIONS, ATOMS), jnp.float32)
    return jax.nn.softmax(scores, axis=-1)


def with_ends(values, key, low, top_value):
    spot = [jax.random.randint(jax.random.fold_in(key, axis), (), 0, length) for axis, length in enumerate(values.shape)]
    widest = values.shape.index(max(values.shape))
    beside = spot[:widest] + [(spot[widest] + 1) % values.shape[widest]] + spot[widest + 1:]
    return values.at[tuple(spot)].set(low).at[tuple(beside)].set(top_value)


def levels(key, dims, pieces, smallest, high):
    def one(dim, parts):
        heights = jax.random.uniform(jax.random.fold_in(jax.random.fold_in(key, 6), dim), (parts,), jnp.float32, smallest / len(pieces), high / len(pieces))
        return jnp.repeat(jnp.exp(heights), dims[dim] // parts).reshape((-1,) + (1,) * (len(dims) - dim - 1))

    gain = one(*pieces[0])
    for cut in pieces[1:]:
        gain = gain * one(*cut)
    return gain


def scatter_about(key, shape, width, bound, cuts=(), held_as=jnp.bfloat16):
    drawn = width * jax.random.normal(key, shape, jnp.float32)
    if cuts:
        drawn = drawn * levels(key, shape, cuts, -0.22, 0.18)
    return jnp.clip(drawn, -bound, bound).astype(held_as)


def setup_inputs(seed: int = 0) -> dict:
    arg_keys = jax.random.split(jax.random.key(seed), 12)
    return {
        "features": scatter_about(arg_keys[0], (TOTAL, FEAT), 1.0, 6.0, ((0, 128),)),
        "w_one": scatter_about(arg_keys[1], (HID, FEAT), FEAT ** -0.5, 0.109375),
        "b_one": scatter_about(arg_keys[2], (HID,), 0.5, 3.0, (), jnp.float32),
        "w_two": scatter_about(arg_keys[3], (HID, ACTIONS * ATOMS), HID ** -0.5, 0.25),
        "b_two": draw_b_two(jax.random.fold_in(arg_keys[11], 71), 0),
        "action": with_ends(jax.random.randint(arg_keys[5], (TOTAL,), 0, ACTIONS), jax.random.fold_in(arg_keys[5], 1), 0, ACTIONS - 1).astype(jnp.int32),
        "target_probs": draw_target_probs(jax.random.fold_in(arg_keys[11], 71), 0),
        "next_action": with_ends(jax.random.randint(arg_keys[7], (TOTAL,), 0, ACTIONS), jax.random.fold_in(arg_keys[7], 1), 0, ACTIONS - 1).astype(jnp.int32),
        "lower_idx": with_ends(jax.random.randint(arg_keys[8], (TOTAL, ATOMS), 0, ATOMS - 1), jax.random.fold_in(arg_keys[8], 1), 0, (ATOMS - 1) - 1).astype(jnp.int32),
        "upper_frac": jnp.clip(1.0 * jax.random.uniform(arg_keys[9], (TOTAL, ATOMS), jnp.float32) ** levels(arg_keys[9], (TOTAL, ATOMS), ((0, 128),), -0.2, 0.2), 0.0, 1.0),
        "is_weight": jnp.clip(jnp.exp(math.log(1.0) - 2.3025851 * jax.random.uniform(arg_keys[10], (TOTAL,), jnp.float32) ** levels(arg_keys[10], (TOTAL,), ((0, 128),), -0.2, 0.2)), 0.1, 1.0),
    }


def forward_loss(features, w_one, b_one, w_two, b_two, action, target_probs, next_action, lower_idx, upper_frac, is_weight):
    row_count = features.shape[0]
    n_act = target_probs.shape[1]
    n_atom = target_probs.shape[2]
    pre_act = lax.dot_general(features, w_one, (((1,), (1,)), ((), ())), preferred_element_type=jnp.float32) + b_one
    hidden = jnp.maximum(pre_act, 0.0).astype(jnp.bfloat16)
    logits = (jnp.dot(hidden, w_two, preferred_element_type=jnp.float32) + b_two).reshape(row_count, n_act, n_atom)
    chosen = jnp.take_along_axis(logits, action.astype(jnp.int32)[:, None, None], axis=1)[:, 0, :]
    log_probs = jax.nn.log_softmax(chosen, axis=-1)
    next_probs = jnp.take_along_axis(target_probs, next_action.astype(jnp.int32)[:, None, None], axis=1)[:, 0, :]
    atom_ids = jnp.arange(n_atom, dtype=jnp.int32)
    mass_low = next_probs * (1.0 - upper_frac)
    mass_high = next_probs * upper_frac
    low_hot = lower_idx[:, :, None] == atom_ids[None, None, :]
    high_hot = (lower_idx[:, :, None] + 1) == atom_ids[None, None, :]
    projected = jnp.sum(jnp.where(low_hot, mass_low[:, :, None], 0.0) + jnp.where(high_hot, mass_high[:, :, None], 0.0), axis=1)
    cross_ent = -jnp.sum(projected * log_probs, axis=-1)
    grad_chosen = is_weight[:, None] * (jnp.exp(log_probs) * jnp.sum(projected, axis=-1, keepdims=True) - projected)
    act_hot = action[:, None] == jnp.arange(n_act, dtype=jnp.int32)[None, :]
    grad_logits = jnp.where(act_hot[:, :, None], grad_chosen[:, None, :], 0.0).reshape(row_count, n_act * n_atom).astype(jnp.bfloat16)
    grad_hidden = lax.dot_general(grad_logits, w_two, (((1,), (1,)), ((), ())), preferred_element_type=jnp.float32)
    grad_pre = jnp.where(pre_act > 0.0, grad_hidden, 0.0).astype(jnp.bfloat16)
    return hidden, grad_logits, grad_pre, cross_ent


def reference(features, w_one, b_one, w_two, b_two, action, target_probs, next_action, lower_idx, upper_frac, is_weight):
    def split_rows(array):
        return array.reshape((N_DP, ROWS) + array.shape[1:])

    blocks = tuple(split_rows(item) for item in (features, action, target_probs, next_action, lower_idx, upper_frac, is_weight))

    def step(carry, block):
        g_w1, g_b1, g_w2, g_b2, loss_sum, top = carry
        feat, act, probs, nxt, lower, frac, weight = block
        hidden, grad_logits, grad_pre, cross_ent = forward_loss(feat, w_one, b_one, w_two, b_two, act, probs, nxt, lower, frac, weight)
        g_w1 = g_w1 + lax.dot_general(grad_pre, feat, (((0,), (0,)), ((), ())), preferred_element_type=jnp.float32)
        g_b1 = g_b1 + jnp.sum(grad_pre.astype(jnp.float32), axis=0)
        g_w2 = g_w2 + lax.dot_general(hidden, grad_logits, (((0,), (0,)), ((), ())), preferred_element_type=jnp.float32)
        g_b2 = g_b2 + jnp.sum(grad_logits.astype(jnp.float32), axis=0)
        loss_sum = loss_sum + jnp.sum(weight * cross_ent)
        top = jnp.maximum(top, jnp.max(cross_ent))
        return (g_w1, g_b1, g_w2, g_b2, loss_sum, top), cross_ent

    start = (jnp.zeros(w_one.shape, jnp.float32), jnp.zeros(b_one.shape, jnp.float32),
             jnp.zeros(w_two.shape, jnp.float32), jnp.zeros(b_two.shape, jnp.float32),
             jnp.zeros((), jnp.float32), jnp.zeros((), jnp.float32))
    (g_w1, g_b1, g_w2, g_b2, loss_sum, top), losses = lax.scan(step, start, blocks)
    priorities = losses.reshape(-1) / jnp.maximum(top, 1.0)
    mean_loss = loss_sum / TOTAL
    return g_w1, g_b1, g_w2, g_b2, mean_loss, priorities
```

```python
import functools

import jax
import jax.numpy as jnp
from jax import lax
from jax.experimental import pallas as pl
from jax.experimental.pallas import tpu as pltpu
from jax.sharding import PartitionSpec as P

MESH = pl.DeviceIdType.MESH
F32, BF16 = jnp.float32, jnp.bfloat16

FEAT, HID, ACT, ATOM, ROWS = 3136, 512, 18, 51, 1024
SLOT = 64
HEAD = ACT * SLOT
HEADS = ACT * ATOM

W2_AT = FEAT
B1_AT = W2_AT + HEADS
B2_AT = B1_AT + 1
TOP_AT = B2_AT + 2
LOSS_AT = TOP_AT + 1
TOTAL_ROWS = 4096
HALF = TOTAL_ROWS // 2
STREAMS = ((0, 640), (640, 640), (1280, 768))


def compute_kernel(
    feat_hbm, w1_hbm, b1_hbm, w2_hbm, b2_hbm, act_hbm, tp_hbm, nact_hbm, low_hbm, frac_hbm, isw_hbm,
    part_ref, ce_ref,
    feat, w1, b1_ref, w2raw, b2_ref, act_ref, tp, nact_ref, low_ref, frac_ref, isw_ref,
    w2f, w2p, b2col, mlow, mhigh, proj, hid, glt, gp, gb2, sems,
):
    me = lax.axis_index("dp")
    pairs = [
        (w2_hbm, w2raw), (b2_hbm, b2_ref), (nact_hbm, nact_ref), (low_hbm, low_ref), (frac_hbm, frac_ref),
        (tp_hbm, tp), (w1_hbm, w1), (b1_hbm, b1_ref), (feat_hbm, feat), (act_hbm, act_ref), (isw_hbm, isw_ref),
    ]
    copies = [pltpu.make_async_copy(src, dst, sems.at[i]) for i, (src, dst) in enumerate(pairs)]
    for copy in copies:
        copy.start()

    copies[0].wait()
    copies[1].wait()
    w2f[...] = w2raw[...].astype(F32)
    wrow = lax.broadcasted_iota(jnp.int32, (SLOT, HID), 0)
    for a in range(ACT):
        if a < ACT - 1:
            block = w2f[ATOM * a : ATOM * a + SLOT, :]
        else:
            block = jnp.concatenate([w2f[ATOM * a : HEADS, :], jnp.zeros((SLOT - ATOM, HID), F32)], axis=0)
        w2p[SLOT * a : SLOT * (a + 1), :] = jnp.where(wrow < ATOM, block, 0.0).astype(BF16)
    b2row = jnp.concatenate([b2_ref[...], jnp.zeros((1, 1024 - HEADS), F32)], axis=1)
    b2col[0:1024, :] = jnp.broadcast_to(b2row, (128, 1024)).T
    b2col[1024:, :] = jnp.zeros((64, 128), F32)

    for copy in copies[2:6]:
        copy.wait()
    atom_row = lax.broadcasted_iota(jnp.int32, (SLOT, 128), 0)

    def project(t, carry):
        lanes = pl.ds(pl.multiple_of(t * 128, 128), 128)
        nact = nact_ref[:, lanes]
        probs = jnp.zeros((ATOM, 128), F32)
        for a in range(ACT):
            probs = jnp.where(nact == a, tp[a, :, lanes], probs)
        frac = frac_ref[:, lanes]
        mlow[...] = probs * (1.0 - frac)
        mhigh[...] = probs * frac
        low_sum = jnp.zeros((SLOT, 128), F32)
        high_sum = jnp.zeros((SLOT, 128), F32)
        for j in range(ATOM):
            hot = low_ref[pl.ds(j, 1), lanes] == atom_row
            low_sum = low_sum + jnp.where(hot, mlow[pl.ds(j, 1), :], 0.0)
            high_sum = high_sum + jnp.where(hot, mhigh[pl.ds(j, 1), :], 0.0)
        high_sum = jnp.where(atom_row == 0, 0.0, pltpu.roll(high_sum, 1, 0))
        proj[:, lanes] = low_sum + high_sum
        return carry

    lax.fori_loop(0, ROWS // 128, project, 0)

    for copy in copies[6:]:
        copy.wait()

    def forward(t, carry):
        cols = pl.ds(pl.multiple_of(t * 256, 256), 256)
        pre = lax.dot_general(feat[:, cols], w1[...], (((0,), (0,)), ((), ())), preferred_element_type=F32)
        hid[cols, :] = jnp.maximum(pre + b1_ref[...], 0.0).astype(BF16)
        return carry

    lax.fori_loop(0, ROWS // 256, forward, 0)

    valid = lax.broadcasted_iota(jnp.int32, (SLOT, 256), 0) < ATOM

    def head(t, carry):
        loss, top = carry
        cols = pl.ds(pl.multiple_of(t * 256, 256), 256)
        logits = lax.dot_general(w2p[...], hid[cols, :], (((1,), (1,)), ((), ())), preferred_element_type=F32)
        action = act_ref[:, cols]
        chosen = jnp.zeros((SLOT, 256), F32)
        for a in range(ACT):
            bias = b2col[ATOM * a : ATOM * a + SLOT, :]
            biased = logits[SLOT * a : SLOT * (a + 1), :] + jnp.concatenate([bias, bias], axis=1)
            chosen = jnp.where(action == a, biased, chosen)
        chosen = jnp.where(valid, chosen, -1e30)
        shifted = chosen - jnp.max(chosen, axis=0, keepdims=True)
        expd = jnp.where(valid, jnp.exp(shifted), 0.0)
        log_probs = shifted - jnp.log(jnp.sum(expd, axis=0, keepdims=True))
        projected = proj[:, cols]
        cross = -jnp.sum(jnp.where(valid, projected * log_probs, 0.0), axis=0, keepdims=True)
        weight = isw_ref[:, cols]
        probs = jnp.where(valid, jnp.exp(log_probs), 0.0)
        grad = weight * (probs * jnp.sum(projected, axis=0, keepdims=True) - projected)
        grad16 = grad.astype(BF16)
        for a in range(ACT):
            glt[SLOT * a : SLOT * (a + 1), cols] = jnp.where(action == a, grad, 0.0).astype(BF16)
        ce_ref[:, cols] = cross
        return loss + weight * cross, jnp.maximum(top, cross)

    loss_row, top_row = lax.fori_loop(
        0, ROWS // 256, head, (jnp.zeros((1, 256), F32), jnp.full((1, 256), -jnp.inf, F32))
    )

    def back(t, gb1):
        cols = pl.ds(pl.multiple_of(t * 256, 256), 256)
        gh = lax.dot_general(glt[:, cols], w2p[...], (((0,), (0,)), ((), ())), preferred_element_type=F32)
        g16 = jnp.where(hid[cols, :].astype(F32) > 0.0, gh, 0.0).astype(BF16)
        gp[cols, :] = g16
        return gb1 + jnp.sum(g16.astype(F32), axis=0, keepdims=True)

    gb1 = lax.fori_loop(0, ROWS // 256, back, jnp.zeros((1, HID), F32))

    group = 6
    for g in range(ACT // group):
        rows = group * SLOT
        gl = glt[g * rows : (g + 1) * rows, :]
        gw2 = lax.dot_general(gl, hid[...], (((1,), (0,)), ((), ())), preferred_element_type=F32)
        for i in range(group):
            a = g * group + i
            part_ref[W2_AT + ATOM * a : W2_AT + ATOM * (a + 1), :] = gw2[SLOT * i : SLOT * i + ATOM, :]
            ga = glt[SLOT * a : SLOT * (a + 1), :].astype(F32)
            gb2[ATOM * a : ATOM * (a + 1), :] = jnp.broadcast_to(jnp.sum(ga, axis=1, keepdims=True), (SLOT, 128))[:ATOM]
    gb2[HEADS:, :] = jnp.zeros((1024 - HEADS, 128), F32)
    gb2_row = gb2[...].T[0:1, :]

    lane = lax.broadcasted_iota(jnp.int32, (1, HID), 1)
    top = jnp.max(top_row)
    loss = jnp.sum(loss_row)
    tail = jnp.concatenate(
        [
            gb1,
            gb2_row[:, :HID],
            gb2_row[:, HID:],
            jnp.where(lane == me, top, 0.0),
            jnp.where(lane == 0, loss, 0.0),
            jnp.zeros((TOTAL_ROWS - LOSS_AT - 1, HID), F32),
        ],
        axis=0,
    )
    part_ref[B1_AT:, :] = tail

    def grad_w1(i, carry):
        rows = pl.ds(pl.multiple_of(i * 448, 64), 448)
        part_ref[rows, :] = jnp.dot(feat[rows, :], gp[...], preferred_element_type=F32)
        return carry

    lax.fori_loop(0, FEAT // 448, grad_w1, 0)


def compute(feat, w1, b1, w2, b2, action, tp, naction, low, frac, isw):
    any_spec = pl.BlockSpec(memory_space=pltpu.HBM)
    vm = pl.BlockSpec(memory_space=pltpu.VMEM)
    return pl.pallas_call(
        compute_kernel,
        name="compute",
        in_specs=[any_spec] * 11,
        out_specs=[vm, vm],
        out_shape=[pltpu.VMEM((TOTAL_ROWS, HID), F32), pltpu.VMEM((1, ROWS), F32)],
        scratch_shapes=[
            pltpu.VMEM((FEAT, ROWS), BF16),
            pltpu.VMEM((FEAT, HID), BF16),
            pltpu.VMEM((1, HID), F32),
            pltpu.VMEM((HEADS, HID), BF16),
            pltpu.VMEM((1, HEADS), F32),
            pltpu.VMEM((1, ROWS), jnp.int32),
            pltpu.VMEM((ACT, ATOM, ROWS), F32),
            pltpu.VMEM((1, ROWS), jnp.int32),
            pltpu.VMEM((ATOM, ROWS), jnp.int32),
            pltpu.VMEM((ATOM, ROWS), F32),
            pltpu.VMEM((1, ROWS), F32),
            pltpu.VMEM((HEADS, HID), F32),
            pltpu.VMEM((HEAD, HID), BF16),
            pltpu.VMEM((1088, 128), F32),
            pltpu.VMEM((ATOM, 128), F32),
            pltpu.VMEM((ATOM, 128), F32),
            pltpu.VMEM((SLOT, ROWS), F32),
            pltpu.VMEM((ROWS, HID), BF16),
            pltpu.VMEM((HEAD, ROWS), BF16),
            pltpu.VMEM((ROWS, HID), BF16),
            pltpu.VMEM((1024, 128), F32),
            pltpu.SemaphoreType.DMA((11,)),
        ],
        compiler_params=pltpu.CompilerParams(vmem_limit_bytes=45 * 1024 * 1024),
    )(feat, w1, b1, w2, b2, action, tp, naction, low, frac, isw)


class Sends:
    def __init__(self, send_sem, recv_sem):
        self.send_sem, self.recv_sem, self.made = send_sem, recv_sem, []

    def __call__(self, src, dst, device):
        i = len(self.made)
        copy = pltpu.make_async_remote_copy(
            src_ref=src, dst_ref=dst, send_sem=self.send_sem.at[i], recv_sem=self.recv_sem.at[i],
            device_id=(device,), device_id_type=MESH,
        )
        copy.start()
        self.made.append(copy)
        return copy


COPIES = 3 * 38
LO, HI = slice(0, HID // 2), slice(HID // 2, HID)


def rows_at(start, size):
    return pl.ds(pl.multiple_of(start, 8), size)


def plan(me, core):
    out = []
    for s in range(3):
        stages = []
        for k in range(3):
            axis = (s + k + core) % 3
            stride = 32 - 33 * axis + 9 * axis * axis
            at = (me // stride) % 4
            ahead = [me + stride * ((at + d) % 4 - at) for d in range(4)]
            stages.append((at, ahead))
        out.append(stages)
    return out


def comm_kernel(part, ce, tot, prio, work, plus_a, minus_a, one_a, plus_b, minus_b, one_b, piece, send_sem, recv_sem):
    me = lax.axis_index("dp")
    core = me % 2
    sibling = me + 1 - 2 * core
    mine, theirs = plan(me, core), plan(me, 1 - core)
    near = [sibling]
    for k in range(3):
        near += mine[0][k][1][1:]
    barrier = pltpu.get_barrier_semaphore()
    for device in near:
        pl.semaphore_signal(barrier, inc=1, device_id=(device,), device_id_type=MESH)
    pl.semaphore_wait(barrier, len(near))

    send = Sends(send_sem, recv_sem)
    base = core * HALF
    other = (1 - core) * HALF
    ORDER = (2, 1, 3, 0)

    swap = {}
    for d in ORDER:
        for s, (first, size) in enumerate(STREAMS):
            q = size // 4
            at = (theirs[s][0][0] + d) % 4 * q + first
            swap[s, d] = send(part.at[rows_at(other + at, q), :], work.at[rows_at(at, q), :], sibling)

    def scatter(k, blocks, sizes, plus, minus, one, before=None):
        copies, quarter = {}, {}
        for d in ORDER:
            for s in range(3):
                at, ahead = mine[s][k]
                q = sizes[s]
                rows = rows_at(blocks[s] + (at + d) % 4 * q, q)
                quarter[s, d] = rows
                if before is not None:
                    before(s, d, rows)
                here = pl.ds(0, q)
                if d == 2:
                    copies[s, "p1"] = send(work.at[rows, LO], one.at[s, here, LO], ahead[1])
                    copies[s, "m1"] = send(work.at[rows, HI], one.at[s, here, HI], ahead[3])
                elif d == 1:
                    copies[s, "p2"] = send(work.at[rows, HI], plus.at[s, here, HI], ahead[1])
                elif d == 3:
                    copies[s, "m2"] = send(work.at[rows, LO], minus.at[s, here, LO], ahead[3])
        for s in range(3):
            at, ahead = mine[s][k]
            here = pl.ds(0, sizes[s])
            copies[s, "p1"].wait_recv()
            rows = quarter[s, 1]
            work[rows, LO] = work[rows, LO] + one[s, here, LO]
            copies[s, "p3"] = send(work.at[rows, LO], plus.at[s, here, LO], ahead[1])
            copies[s, "m1"].wait_recv()
            rows = quarter[s, 3]
            work[rows, HI] = work[rows, HI] + one[s, here, HI]
            copies[s, "m3"] = send(work.at[rows, HI], minus.at[s, here, HI], ahead[3])
        for s in range(3):
            here = pl.ds(0, sizes[s])
            for name in ("p2", "m2", "p3", "m3"):
                copies[s, name].wait_recv()
            rows = quarter[s, 0]
            work[rows, :] = work[rows, :] + (plus[s, here, :] + minus[s, here, :])
        return [blocks[s] + mine[s][k][0] * sizes[s] for s in range(3)]

    def add_own(s, d, rows):
        q = STREAMS[s][1] // 4
        at = (mine[s][0][0] + d) % 4 * q + STREAMS[s][0]
        swap[s, d].wait_recv()
        work[rows, :] = work[rows, :] + part[rows_at(base + at, q), :]

    size_a = [size // 4 for _, size in STREAMS]
    size_b = [size // 16 for _, size in STREAMS]
    block_a = [first for first, _ in STREAMS]
    block_b = scatter(0, block_a, size_a, plus_a, minus_a, one_a, add_own)
    block_c = scatter(1, block_b, size_b, plus_b, minus_b, one_b)

    def lanes_at(p):
        return pl.ds(pl.multiple_of(p * 128, 128), 128)

    last = {}
    for d in (2, 1, 3):
        for s in range(3):
            at, ahead = mine[s][2]
            last[s, d] = send(
                work.at[rows_at(block_c[s], size_b[s]), lanes_at((at + d) % 4)],
                piece.at[s, d - 1, pl.ds(0, size_b[s]), :], ahead[d],
            )
    final = {}
    for s in range(3):
        at, ahead = mine[s][2]
        here = pl.ds(0, size_b[s])
        for d in (1, 3, 2):
            last[s, d].wait_recv()
        got = work[rows_at(block_c[s], size_b[s]), lanes_at(at)] + (piece[s, 0, here, :] + piece[s, 2, here, :])
        rows = rows_at(base + block_c[s], size_b[s])
        tot[rows, lanes_at(at)] = got + piece[s, 1, here, :]
        for d in (2, 1, 3):
            ref = tot.at[rows, lanes_at(at)]
            final[s, d] = send(ref, ref, ahead[d])
    for s in range(3):
        for d in (1, 3, 2):
            final[s, d].wait_recv()

    def gather(k, blocks, sizes, pair):
        copies, pairs = {}, []

        def rows_of(s, d):
            return rows_at(base + blocks[s] + (mine[s][k][0] + d) % 4 * sizes[s], sizes[s])

        def put(s, d, lanes, device):
            ref = tot.at[rows_of(s, d), lanes]
            return send(ref, ref, device)

        def to_sibling(s, d):
            if pair:
                pairs.append(put(s, d, slice(0, HID), sibling))

        for s in range(3):
            ahead = mine[s][k][1]
            copies[s, "p1"] = put(s, 0, LO, ahead[1])
            copies[s, "m1"] = put(s, 0, HI, ahead[3])
            copies[s, "p2"] = put(s, 0, HI, ahead[1])
            copies[s, "m2"] = put(s, 0, LO, ahead[3])
        for s in range(3):
            to_sibling(s, 0)
        for s in range(3):
            ahead = mine[s][k][1]
            copies[s, "p1"].wait_recv()
            copies[s, "p3"] = put(s, 3, LO, ahead[1])
            copies[s, "m1"].wait_recv()
            copies[s, "m3"] = put(s, 1, HI, ahead[3])
        for s in range(3):
            copies[s, "p2"].wait_recv()
            to_sibling(s, 3)
            copies[s, "m2"].wait_recv()
            to_sibling(s, 1)
        for s in range(3):
            copies[s, "p3"].wait_recv()
            copies[s, "m3"].wait_recv()
            to_sibling(s, 2)
        for copy in pairs:
            copy.wait_recv()

    gather(1, block_b, size_b, False)
    gather(0, block_a, size_a, True)
    for copy in send.made:
        copy.wait_send()
    top = jnp.max(tot[TOP_AT : TOP_AT + 1, 0:128])
    prio[...] = ce[...] / jnp.maximum(top, 1.0)


def all_sum(part, ce):
    vm = pl.BlockSpec(memory_space=pltpu.VMEM)
    q = STREAMS[2][1] // 4
    return pl.pallas_call(
        comm_kernel,
        name="all_sum",
        in_specs=[vm, vm],
        out_specs=[vm, vm],
        out_shape=[pltpu.VMEM((TOTAL_ROWS, HID), F32), pltpu.VMEM((1, ROWS), F32)],
        scratch_shapes=[
            pltpu.VMEM((HALF, HID), F32),
            pltpu.VMEM((3, q, HID), F32),
            pltpu.VMEM((3, q, HID), F32),
            pltpu.VMEM((3, q, HID), F32),
            pltpu.VMEM((3, q // 4, HID), F32),
            pltpu.VMEM((3, q // 4, HID), F32),
            pltpu.VMEM((3, q // 4, HID), F32),
            pltpu.VMEM((3, 3, q // 4, 128), F32),
            pltpu.SemaphoreType.DMA((COPIES,)),
            pltpu.SemaphoreType.DMA((COPIES,)),
        ],
        compiler_params=pltpu.CompilerParams(
            vmem_limit_bytes=16 * 1024 * 1024, collective_id=0, has_side_effects=True
        ),
    )(part, ce)


def on_device(features, w_one, b_one, w_two, b_two, action, target_probs, next_action, lower_idx, upper_frac, is_weight):
    part, ce = compute(
        features.T, w_one.T, b_one[None, :], w_two.T, b_two[None, :], action[None, :],
        target_probs.transpose(1, 2, 0), next_action[None, :], lower_idx.T, upper_frac.T, is_weight[None, :],
    )
    total, prio = all_sum(part, ce)
    return (
        total[:FEAT].T,
        total[B1_AT],
        total[W2_AT:B1_AT].T,
        total[B2_AT : B2_AT + 2].reshape(-1)[:HEADS],
        total[LOSS_AT, 0] / (ROWS * lax.axis_size("dp")),
        prio[0],
    )


def solution(mesh):
    in_specs = (
        P("dp", None), P(), P(), P(), P(), P("dp"), P("dp", None, None), P("dp"), P("dp", None), P("dp", None), P("dp"),
    )
    out_specs = (P(), P(), P(), P(), P(), P("dp"))
    return jax.shard_map(on_device, mesh=mesh, in_specs=in_specs, out_specs=out_specs, check_vma=False)
```

```python
import functools

import jax
import jax.numpy as jnp
from jax import lax
from jax.experimental import pallas as pl
from jax.experimental.pallas import tpu as pltpu
from jax.sharding import PartitionSpec as P

MESH = pl.DeviceIdType.MESH
F32, BF16 = jnp.float32, jnp.bfloat16

FEAT, HID, ACT, ATOM, ROWS = 3136, 512, 18, 51, 1024
SLOT = 64
HEAD = ACT * SLOT
HEADS = ACT * ATOM

W1_AT = 928
B1_AT = W1_AT + FEAT
B2_AT = B1_AT + 1
TOP_AT = B2_AT + 2
LOSS_AT = TOP_AT + 1
TOTAL_ROWS = 4096
WAVES = ((128, 128, 128), (256, 256, 256), (256, 256, 384))


def main_kernel(
    feat_hbm, w1_hbm, b1_hbm, w2_hbm, b2_hbm, act_hbm, tp_hbm, nact_hbm, low_hbm, frac_hbm, isw_hbm,
    tot, ce_ref,
    feat, w1, b1_ref, w2raw, b2_ref, act_ref, tp, nact_ref, low_ref, frac_ref, isw_ref,
    w2f, w2p, b2col, mlow, mhigh, proj, hid, glt, gp, gb2, part_ref, sems, send_sem, recv_sem, *buffers,
):
    me = lax.axis_index("dp")
    core = me % 2
    sibling = me + 1 - 2 * core
    pairs = [
        (w2_hbm, w2raw), (b2_hbm, b2_ref), (nact_hbm, nact_ref), (low_hbm, low_ref), (frac_hbm, frac_ref),
        (tp_hbm, tp), (w1_hbm, w1), (b1_hbm, b1_ref), (feat_hbm, feat), (act_hbm, act_ref), (isw_hbm, isw_ref),
    ]
    copies = [pltpu.make_async_copy(src, dst, sems.at[i]) for i, (src, dst) in enumerate(pairs)]
    for copy in copies:
        copy.start()
    near = [sibling]
    for axis in range(3):
        near += ring(me, axis)[1][1:]
    barrier = pltpu.get_barrier_semaphore()
    for device in near:
        pl.semaphore_signal(barrier, inc=1, device_id=(device,), device_id_type=MESH)

    copies[0].wait()
    copies[1].wait()
    w2f[...] = w2raw[...].astype(F32)
    wrow = lax.broadcasted_iota(jnp.int32, (SLOT, HID), 0)
    for a in range(ACT):
        if a < ACT - 1:
            block = w2f[ATOM * a : ATOM * a + SLOT, :]
        else:
            block = jnp.concatenate([w2f[ATOM * a : HEADS, :], jnp.zeros((SLOT - ATOM, HID), F32)], axis=0)
        w2p[SLOT * a : SLOT * (a + 1), :] = jnp.where(wrow < ATOM, block, 0.0).astype(BF16)
    b2row = jnp.concatenate([b2_ref[...], jnp.zeros((1, 1024 - HEADS), F32)], axis=1)
    b2col[0:1024, :] = jnp.broadcast_to(b2row, (128, 1024)).T
    b2col[1024:, :] = jnp.zeros((64, 128), F32)

    for copy in copies[2:6]:
        copy.wait()
    atom_row = lax.broadcasted_iota(jnp.int32, (SLOT, 128), 0)

    def project(t, carry):
        lanes = pl.ds(pl.multiple_of(t * 128, 128), 128)
        nact = nact_ref[:, lanes]
        probs = jnp.zeros((ATOM, 128), F32)
        for a in range(ACT):
            probs = jnp.where(nact == a, tp[a, :, lanes], probs)
        frac = frac_ref[:, lanes]
        mlow[...] = probs * (1.0 - frac)
        mhigh[...] = probs * frac
        low_sum = jnp.zeros((SLOT, 128), F32)
        high_sum = jnp.zeros((SLOT, 128), F32)
        for j in range(ATOM):
            hot = low_ref[pl.ds(j, 1), lanes] == atom_row
            low_sum = low_sum + jnp.where(hot, mlow[pl.ds(j, 1), :], 0.0)
            high_sum = high_sum + jnp.where(hot, mhigh[pl.ds(j, 1), :], 0.0)
        high_sum = jnp.where(atom_row == 0, 0.0, pltpu.roll(high_sum, 1, 0))
        proj[:, lanes] = low_sum + high_sum
        return carry

    lax.fori_loop(0, ROWS // 128, project, 0)

    for copy in copies[6:]:
        copy.wait()

    def forward(t, carry):
        cols = pl.ds(pl.multiple_of(t * 256, 256), 256)
        pre = lax.dot_general(feat[:, cols], w1[...], (((0,), (0,)), ((), ())), preferred_element_type=F32)
        hid[cols, :] = jnp.maximum(pre + b1_ref[...], 0.0).astype(BF16)
        return carry

    lax.fori_loop(0, ROWS // 256, forward, 0)

    valid = lax.broadcasted_iota(jnp.int32, (SLOT, 256), 0) < ATOM

    def head(t, carry):
        loss, top = carry
        cols = pl.ds(pl.multiple_of(t * 256, 256), 256)
        logits = lax.dot_general(w2p[...], hid[cols, :], (((1,), (1,)), ((), ())), preferred_element_type=F32)
        action = act_ref[:, cols]
        chosen = jnp.zeros((SLOT, 256), F32)
        for a in range(ACT):
            bias = b2col[ATOM * a : ATOM * a + SLOT, :]
            biased = logits[SLOT * a : SLOT * (a + 1), :] + jnp.concatenate([bias, bias], axis=1)
            chosen = jnp.where(action == a, biased, chosen)
        chosen = jnp.where(valid, chosen, -1e30)
        shifted = chosen - jnp.max(chosen, axis=0, keepdims=True)
        expd = jnp.where(valid, jnp.exp(shifted), 0.0)
        log_probs = shifted - jnp.log(jnp.sum(expd, axis=0, keepdims=True))
        projected = proj[:, cols]
        cross = -jnp.sum(jnp.where(valid, projected * log_probs, 0.0), axis=0, keepdims=True)
        weight = isw_ref[:, cols]
        probs = jnp.where(valid, jnp.exp(log_probs), 0.0)
        grad = weight * (probs * jnp.sum(projected, axis=0, keepdims=True) - projected)
        grad16 = grad.astype(BF16)
        for a in range(ACT):
            glt[SLOT * a : SLOT * (a + 1), cols] = jnp.where(action == a, grad, 0.0).astype(BF16)
        ce_ref[:, cols] = cross
        return loss + weight * cross, jnp.maximum(top, cross)

    loss_row, top_row = lax.fori_loop(
        0, ROWS // 256, head, (jnp.zeros((1, 256), F32), jnp.full((1, 256), -jnp.inf, F32))
    )

    group = 6
    for g in range(ACT // group):
        rows = group * SLOT
        gl = glt[g * rows : (g + 1) * rows, :]
        gw2 = lax.dot_general(gl, hid[...], (((1,), (0,)), ((), ())), preferred_element_type=F32)
        for i in range(group):
            a = g * group + i
            part_ref[ATOM * a : ATOM * (a + 1), :] = gw2[SLOT * i : SLOT * i + ATOM, :]
    part_ref[HEADS:W1_AT, :] = jnp.zeros((W1_AT - HEADS, HID), F32)

    pl.semaphore_wait(barrier, len(near))
    send = Sends(send_sem, recv_sem)
    waves, row, at = [], 0, 0
    for i, sizes in enumerate(WAVES):
        waves.append(Wave(i, sizes, row, me, core, send, part_ref, tot, buffers[8 * i : 8 * (i + 1)]))
        row += 2 * sum(sizes)
    assert row == TOTAL_ROWS
    wave0, wave1, wave2 = waves
    wave0.swap()

    for a in range(ACT):
        ga = glt[SLOT * a : SLOT * (a + 1), :].astype(F32)
        gb2[ATOM * a : ATOM * (a + 1), :] = jnp.broadcast_to(jnp.sum(ga, axis=1, keepdims=True), (SLOT, 128))[:ATOM]
    gb2[HEADS:, :] = jnp.zeros((1024 - HEADS, 128), F32)
    gb2_row = gb2[...].T[0:1, :]

    def back(t, gb1):
        cols = pl.ds(pl.multiple_of(t * 256, 256), 256)
        gh = lax.dot_general(glt[:, cols], w2p[...], (((0,), (0,)), ((), ())), preferred_element_type=F32)
        g16 = jnp.where(hid[cols, :].astype(F32) > 0.0, gh, 0.0).astype(BF16)
        gp[cols, :] = g16
        return gb1 + jnp.sum(g16.astype(F32), axis=0, keepdims=True)

    gb1 = lax.fori_loop(0, ROWS // 256, back, jnp.zeros((1, HID), F32))

    lane = lax.broadcasted_iota(jnp.int32, (1, HID), 1)
    top = jnp.max(top_row)
    loss = jnp.sum(loss_row)
    part_ref[B1_AT:, :] = jnp.concatenate(
        [
            gb1,
            gb2_row[:, :HID],
            gb2_row[:, HID:],
            jnp.where(lane == me, top, 0.0),
            jnp.where(lane == 0, loss, 0.0),
            jnp.zeros((TOTAL_ROWS - LOSS_AT - 1, HID), F32),
        ],
        axis=0,
    )

    def grad_w1(wave, half, tiles, size):
        low = wave.row + half * wave.half
        start = jnp.maximum(low - W1_AT, 0)
        span = jnp.minimum(low + wave.half - W1_AT, FEAT) - start

        def tile(i, carry):
            at = start + jnp.minimum(i * size, span - size)
            rows = pl.ds(pl.multiple_of(at, 16), size)
            out = pl.ds(pl.multiple_of(at + W1_AT, 16), size)
            part_ref[out, :] = jnp.dot(feat[rows, :], gp[...], preferred_element_type=F32)
            return carry

        lax.fori_loop(0, tiles, tile, 0)

    steps = [wave.steps() for wave in waves]

    def go(text):
        for digit in text:
            next(steps[int(digit)])

    go("0")
    grad_w1(wave1, 1 - core, 3, 256)
    wave1.swap()
    go("0")
    grad_w1(wave1, core, 3, 256)
    go("10")
    grad_w1(wave2, 1 - core, 4, 224)
    wave2.swap()
    go("01")
    grad_w1(wave2, core, 4, 224)
    go("2" + SCHEDULE)
    for copy in send.made:
        copy.wait_send()


def finish_kernel(
    tot, ce, w1_out, b1_out, w2_out, b2_out, loss_out, prio, w2_copy, sems,
):
    first = pltpu.make_async_copy(tot.at[W1_AT:B1_AT, :], w1_out, sems.at[0])
    first.start()
    w2_copy[...] = tot[:HEADS, :]
    second = pltpu.make_async_copy(w2_copy, w2_out, sems.at[1])
    second.start()
    b1_out[...] = tot[B1_AT : B1_AT + 1, :]
    b2_out[...] = jnp.concatenate([tot[B2_AT : B2_AT + 1, :], tot[B2_AT + 1 : B2_AT + 2, :]], axis=1)[:, :HEADS]
    loss_out[...] = tot[LOSS_AT : LOSS_AT + 1, 0:1] * (1.0 / (ROWS * 128))
    top = jnp.max(tot[TOP_AT : TOP_AT + 1, 0:128])
    prio[...] = ce[...] / jnp.maximum(top, 1.0)
    first.wait()
    second.wait()


SCHEDULE = "01201012012012121020212120122"


class Sends:
    def __init__(self, send_sem, recv_sem):
        self.send_sem, self.recv_sem, self.made = send_sem, recv_sem, []

    def __call__(self, src, dst, device):
        i = len(self.made)
        copy = pltpu.make_async_remote_copy(
            src_ref=src, dst_ref=dst, send_sem=self.send_sem.at[i], recv_sem=self.recv_sem.at[i],
            device_id=(device,), device_id_type=MESH,
        )
        copy.start()
        self.made.append(copy)
        return copy


COPIES = len(WAVES) * 3 * 38
LO, HI, ALL = slice(0, HID // 2), slice(HID // 2, HID), slice(0, HID)
ORDER = (2, 1, 3, 0)


def rows_at(start, size):
    return pl.ds(pl.multiple_of(start, 8), size)


def lanes_at(p):
    return pl.ds(pl.multiple_of(p * 128, 128), 128)


def ring(me, axis):
    stride = 32 - 33 * axis + 9 * axis * axis
    at = (me // stride) % 4
    return at, [me + stride * ((at + d) % 4 - at) for d in range(4)]


class Wave:
    def __init__(self, index, sizes, row, me, core, send, part, tot, buffers):
        self.row, self.half, self.send, self.part, self.tot = row, sum(sizes), send, part, tot
        self.work, self.plus_a, self.minus_a, self.one_a, self.plus_b, self.minus_b, self.one_b, self.piece = buffers
        self.sizes = sizes
        self.first = [sum(sizes[:s]) for s in range(3)]
        self.base = row + core * self.half
        self.other = row + (1 - core) * self.half
        self.sibling = me + 1 - 2 * core
        self.mine = [[ring(me, (s + k + core) % 3) for k in range(3)] for s in range(3)]
        self.theirs = [ring(me, (s + 1 - core) % 3)[0] for s in range(3)]

    def swap(self):
        self.swapped = {}
        for d in ORDER:
            for s in range(3):
                q = self.sizes[s] // 4
                at = (self.theirs[s] + d) % 4 * q + self.first[s]
                self.swapped[s, d] = self.send(
                    self.part.at[rows_at(self.other + at, q), :], self.work.at[rows_at(at, q), :], self.sibling
                )

    def scatter(self, k, blocks, sizes, plus, minus, one, first_stage):
        send, work = self.send, self.work
        copies, quarter = {}, {}
        for d in ORDER:
            for s in range(3):
                at, ahead = self.mine[s][k]
                q = sizes[s]
                local = blocks[s] + (at + d) % 4 * q
                rows = rows_at(local, q)
                quarter[s, d] = rows
                if first_stage:
                    self.swapped[s, d].wait_recv()
                    work[rows, :] = work[rows, :] + self.part[rows_at(self.base + local, q), :]
                here = pl.ds(0, q)
                if d == 2:
                    copies[s, "p1"] = send(work.at[rows, LO], one.at[s, here, LO], ahead[1])
                    copies[s, "m1"] = send(work.at[rows, HI], one.at[s, here, HI], ahead[3])
                elif d == 1:
                    copies[s, "p2"] = send(work.at[rows, HI], plus.at[s, here, HI], ahead[1])
                elif d == 3:
                    copies[s, "m2"] = send(work.at[rows, LO], minus.at[s, here, LO], ahead[3])
        yield
        for s in range(3):
            at, ahead = self.mine[s][k]
            here = pl.ds(0, sizes[s])
            copies[s, "p1"].wait_recv()
            rows = quarter[s, 1]
            work[rows, LO] = work[rows, LO] + one[s, here, LO]
            copies[s, "p3"] = send(work.at[rows, LO], plus.at[s, here, LO], ahead[1])
            copies[s, "m1"].wait_recv()
            rows = quarter[s, 3]
            work[rows, HI] = work[rows, HI] + one[s, here, HI]
            copies[s, "m3"] = send(work.at[rows, HI], minus.at[s, here, HI], ahead[3])
        yield
        for s in range(3):
            here = pl.ds(0, sizes[s])
            for name in ("p2", "m2", "p3", "m3"):
                copies[s, name].wait_recv()
            rows = quarter[s, 0]
            work[rows, :] = work[rows, :] + (plus[s, here, :] + minus[s, here, :])

    def gather(self, k, blocks, sizes, pair):
        copies, pairs = {}, []

        def put(s, d, lanes, device):
            start = self.base + blocks[s] + (self.mine[s][k][0] + d) % 4 * sizes[s]
            ref = self.tot.at[rows_at(start, sizes[s]), lanes]
            return self.send(ref, ref, device)

        def to_sibling(s, d):
            if pair:
                pairs.append(put(s, d, ALL, self.sibling))

        for s in range(3):
            ahead = self.mine[s][k][1]
            copies[s, "p1"] = put(s, 0, LO, ahead[1])
            copies[s, "m1"] = put(s, 0, HI, ahead[3])
            copies[s, "p2"] = put(s, 0, HI, ahead[1])
            copies[s, "m2"] = put(s, 0, LO, ahead[3])
        for s in range(3):
            to_sibling(s, 0)
        yield
        for s in range(3):
            ahead = self.mine[s][k][1]
            copies[s, "p1"].wait_recv()
            copies[s, "p3"] = put(s, 3, LO, ahead[1])
            copies[s, "m1"].wait_recv()
            copies[s, "m3"] = put(s, 1, HI, ahead[3])
        yield
        for s in range(3):
            copies[s, "p2"].wait_recv()
            to_sibling(s, 3)
            copies[s, "m2"].wait_recv()
            to_sibling(s, 1)
        for s in range(3):
            copies[s, "p3"].wait_recv()
            copies[s, "m3"].wait_recv()
            to_sibling(s, 2)
        if pair:
            yield
        for copy in pairs:
            copy.wait_recv()

    def steps(self):
        size_a = [size // 4 for size in self.sizes]
        size_b = [size // 16 for size in self.sizes]
        block_a = self.first
        yield from self.scatter(0, block_a, size_a, self.plus_a, self.minus_a, self.one_a, True)
        block_b = [block_a[s] + self.mine[s][0][0] * size_a[s] for s in range(3)]
        yield from self.scatter(1, block_b, size_b, self.plus_b, self.minus_b, self.one_b, False)
        block_c = [block_b[s] + self.mine[s][1][0] * size_b[s] for s in range(3)]

        piece, work, tot = self.piece, self.work, self.tot
        last, final = {}, {}
        for d in (2, 1, 3):
            for s in range(3):
                at, ahead = self.mine[s][2]
                last[s, d] = self.send(
                    work.at[rows_at(block_c[s], size_b[s]), lanes_at((at + d) % 4)],
                    piece.at[s, d - 1, pl.ds(0, size_b[s]), :], ahead[d],
                )
        yield
        for s in range(3):
            at, ahead = self.mine[s][2]
            here = pl.ds(0, size_b[s])
            for d in (1, 3, 2):
                last[s, d].wait_recv()
            got = work[rows_at(block_c[s], size_b[s]), lanes_at(at)] + (piece[s, 0, here, :] + piece[s, 2, here, :])
            rows = rows_at(self.base + block_c[s], size_b[s])
            tot[rows, lanes_at(at)] = got + piece[s, 1, here, :]
            for d in (2, 1, 3):
                ref = tot.at[rows, lanes_at(at)]
                final[s, d] = self.send(ref, ref, ahead[d])
        yield
        for s in range(3):
            for d in (1, 3, 2):
                final[s, d].wait_recv()
        yield from self.gather(1, block_b, size_b, False)
        yield from self.gather(0, block_a, size_a, True)
        yield


def wave_buffers(sizes):
    q, half = max(sizes) // 4, sum(sizes)
    return [
        pltpu.VMEM((half, HID), F32),
        pltpu.VMEM((3, q, HID), F32),
        pltpu.VMEM((3, q, HID), F32),
        pltpu.VMEM((3, q, HID), F32),
        pltpu.VMEM((3, q // 4, HID), F32),
        pltpu.VMEM((3, q // 4, HID), F32),
        pltpu.VMEM((3, q // 4, HID), F32),
        pltpu.VMEM((3, 3, q // 4, 128), F32),
    ]


def in_hbm(x):
    return pltpu.with_memory_space_constraint(x, pltpu.HBM)


def main(*args):
    hbm = pl.BlockSpec(memory_space=pltpu.HBM)
    vm = pl.BlockSpec(memory_space=pltpu.VMEM)
    buffers = []
    for sizes in WAVES:
        buffers += wave_buffers(sizes)
    return pl.pallas_call(
        main_kernel,
        name="gradients_and_sum",
        in_specs=[hbm] * 11,
        out_specs=[vm, vm],
        out_shape=[pltpu.VMEM((TOTAL_ROWS, HID), F32), pltpu.VMEM((1, ROWS), F32)],
        scratch_shapes=[
            pltpu.VMEM((FEAT, ROWS), BF16),
            pltpu.VMEM((FEAT, HID), BF16),
            pltpu.VMEM((1, HID), F32),
            pltpu.VMEM((HEADS, HID), BF16),
            pltpu.VMEM((1, HEADS), F32),
            pltpu.VMEM((1, ROWS), jnp.int32),
            pltpu.VMEM((ACT, ATOM, ROWS), F32),
            pltpu.VMEM((1, ROWS), jnp.int32),
            pltpu.VMEM((ATOM, ROWS), jnp.int32),
            pltpu.VMEM((ATOM, ROWS), F32),
            pltpu.VMEM((1, ROWS), F32),
            pltpu.VMEM((HEADS, HID), F32),
            pltpu.VMEM((HEAD, HID), BF16),
            pltpu.VMEM((1088, 128), F32),
            pltpu.VMEM((ATOM, 128), F32),
            pltpu.VMEM((ATOM, 128), F32),
            pltpu.VMEM((SLOT, ROWS), F32),
            pltpu.VMEM((ROWS, HID), BF16),
            pltpu.VMEM((HEAD, ROWS), BF16),
            pltpu.VMEM((ROWS, HID), BF16),
            pltpu.VMEM((1024, 128), F32),
            pltpu.VMEM((TOTAL_ROWS, HID), F32),
            pltpu.SemaphoreType.DMA((11,)),
            pltpu.SemaphoreType.DMA((COPIES,)),
            pltpu.SemaphoreType.DMA((COPIES,)),
            *buffers,
        ],
        compiler_params=pltpu.CompilerParams(
            vmem_limit_bytes=54 * 1024 * 1024, collective_id=0, has_side_effects=True
        ),
    )(*[in_hbm(x) for x in args])


def finish(tot, ce):
    hbm = pl.BlockSpec(memory_space=pltpu.HBM)
    vm = pl.BlockSpec(memory_space=pltpu.VMEM)
    return pl.pallas_call(
        finish_kernel,
        name="finish",
        in_specs=[vm, vm],
        out_specs=[hbm, vm, hbm, vm, vm, vm],
        out_shape=[
            jax.ShapeDtypeStruct((FEAT, HID), F32),
            jax.ShapeDtypeStruct((1, HID), F32),
            jax.ShapeDtypeStruct((HEADS, HID), F32),
            jax.ShapeDtypeStruct((1, HEADS), F32),
            jax.ShapeDtypeStruct((1, 1), F32),
            jax.ShapeDtypeStruct((1, ROWS), F32),
        ],
        scratch_shapes=[pltpu.VMEM((HEADS, HID), F32), pltpu.SemaphoreType.DMA((2,))],
        compiler_params=pltpu.CompilerParams(vmem_limit_bytes=8 * 1024 * 1024),
    )(tot, ce)


def on_device(features, w_one, b_one, w_two, b_two, action, target_probs, next_action, lower_idx, upper_frac, is_weight):
    tot, ce = main(
        features.T, w_one.T, b_one[None, :], w_two.T, b_two[None, :], action[None, :],
        target_probs.transpose(1, 2, 0), next_action[None, :], lower_idx.T, upper_frac.T, is_weight[None, :],
    )
    gw1, gb1, gw2, gb2, loss, prio = finish(tot, ce)
    return gw1.T, gb1[0], gw2.T, gb2[0], loss[0, 0], prio[0]


def solution(mesh):
    in_specs = (
        P("dp", None), P(), P(), P(), P(), P("dp"), P("dp", None, None), P("dp"), P("dp", None), P("dp", None), P("dp"),
    )
    out_specs = (P(), P(), P(), P(), P(), P("dp"))
    return jax.shard_map(on_device, mesh=mesh, in_specs=in_specs, out_specs=out_specs, check_vma=False)
```

```python
import functools

import jax
import jax.numpy as jnp
from jax import lax
from jax.experimental import pallas as pl
from jax.experimental.pallas import tpu as pltpu
from jax.sharding import PartitionSpec as P

MESH = pl.DeviceIdType.MESH
F32, BF16 = jnp.float32, jnp.bfloat16

FEAT, HID, ACT, ATOM, ROWS = 3136, 512, 18, 51, 1024
SLOT = 64
HEAD = ACT * SLOT
HEADS = ACT * ATOM

W1_AT = 928
B1_AT = W1_AT + FEAT
B2_AT = B1_AT + 1
TOP_AT = B2_AT + 2
LOSS_AT = TOP_AT + 1
TOTAL_ROWS = 4096
WAVES = ((128, 128, 128), (256, 256, 256), (256, 256, 384))


def main_kernel(
    feat_hbm, w1_hbm, b1_hbm, w2_hbm, b2_hbm, act_hbm, tp_hbm, nact_hbm, low_hbm, frac_hbm, isw_hbm,
    tot, ce_ref,
    feat, w1, b1_ref, w2raw, b2_ref, act_ref, tp, nact_ref, low_ref, frac_ref, isw_ref,
    w2f, w2p, b2col, mlow, mhigh, proj, hid, glt, gp, gb2, part_ref, sems, send_sem, recv_sem, *buffers,
):
    me = lax.axis_index("dp")
    core = me % 2
    sibling = me + 1 - 2 * core
    pairs = [
        (w2_hbm, w2raw), (b2_hbm, b2_ref), (nact_hbm, nact_ref), (low_hbm, low_ref), (frac_hbm, frac_ref),
        (tp_hbm, tp), (w1_hbm, w1), (b1_hbm, b1_ref), (feat_hbm, feat), (act_hbm, act_ref), (isw_hbm, isw_ref),
    ]
    copies = [pltpu.make_async_copy(src, dst, sems.at[i]) for i, (src, dst) in enumerate(pairs)]
    for copy in copies:
        copy.start()
    near = [sibling]
    for axis in range(3):
        near += ring(me, axis)[1][1:]
    barrier = pltpu.get_barrier_semaphore()
    for device in near:
        pl.semaphore_signal(barrier, inc=1, device_id=(device,), device_id_type=MESH)

    copies[0].wait()
    copies[1].wait()
    w2f[...] = w2raw[...].astype(F32)
    wrow = lax.broadcasted_iota(jnp.int32, (SLOT, HID), 0)
    for a in range(ACT):
        if a < ACT - 1:
            block = w2f[ATOM * a : ATOM * a + SLOT, :]
        else:
            block = jnp.concatenate([w2f[ATOM * a : HEADS, :], jnp.zeros((SLOT - ATOM, HID), F32)], axis=0)
        w2p[SLOT * a : SLOT * (a + 1), :] = jnp.where(wrow < ATOM, block, 0.0).astype(BF16)
    b2row = jnp.concatenate([b2_ref[...], jnp.zeros((1, 1024 - HEADS), F32)], axis=1)
    b2col[0:1024, :] = jnp.broadcast_to(b2row, (128, 1024)).T
    b2col[1024:, :] = jnp.zeros((64, 128), F32)

    for copy in copies[2:6]:
        copy.wait()
    atom_row = lax.broadcasted_iota(jnp.int32, (SLOT, 128), 0)

    def project(t, carry):
        lanes = pl.ds(pl.multiple_of(t * 128, 128), 128)
        nact = nact_ref[:, lanes]
        probs = jnp.zeros((ATOM, 128), F32)
        for a in range(ACT):
            probs = jnp.where(nact == a, tp[a, :, lanes], probs)
        frac = frac_ref[:, lanes]
        mlow[...] = probs * (1.0 - frac)
        mhigh[...] = probs * frac
        low_sum = jnp.zeros((SLOT, 128), F32)
        high_sum = jnp.zeros((SLOT, 128), F32)
        for j in range(ATOM):
            hot = low_ref[pl.ds(j, 1), lanes] == atom_row
            low_sum = low_sum + jnp.where(hot, mlow[pl.ds(j, 1), :], 0.0)
            high_sum = high_sum + jnp.where(hot, mhigh[pl.ds(j, 1), :], 0.0)
        high_sum = jnp.where(atom_row == 0, 0.0, pltpu.roll(high_sum, 1, 0))
        proj[:, lanes] = low_sum + high_sum
        return carry

    lax.fori_loop(0, ROWS // 128, project, 0)

    for copy in copies[6:]:
        copy.wait()

    def forward(t, carry):
        cols = pl.ds(pl.multiple_of(t * 256, 256), 256)
        pre = lax.dot_general(feat[:, cols], w1[...], (((0,), (0,)), ((), ())), preferred_element_type=F32)
        hid[cols, :] = jnp.maximum(pre + b1_ref[...], 0.0).astype(BF16)
        return carry

    lax.fori_loop(0, ROWS // 256, forward, 0)

    valid = lax.broadcasted_iota(jnp.int32, (SLOT, 256), 0) < ATOM

    def head(t, carry):
        loss, top = carry
        cols = pl.ds(pl.multiple_of(t * 256, 256), 256)
        logits = lax.dot_general(w2p[...], hid[cols, :], (((1,), (1,)), ((), ())), preferred_element_type=F32)
        action = act_ref[:, cols]
        chosen = jnp.zeros((SLOT, 256), F32)
        for a in range(ACT):
            bias = b2col[ATOM * a : ATOM * a + SLOT, :]
            biased = logits[SLOT * a : SLOT * (a + 1), :] + jnp.concatenate([bias, bias], axis=1)
            chosen = jnp.where(action == a, biased, chosen)
        chosen = jnp.where(valid, chosen, -1e30)
        shifted = chosen - jnp.max(chosen, axis=0, keepdims=True)
        expd = jnp.where(valid, jnp.exp(shifted), 0.0)
        log_probs = shifted - jnp.log(jnp.sum(expd, axis=0, keepdims=True))
        projected = proj[:, cols]
        cross = -jnp.sum(jnp.where(valid, projected * log_probs, 0.0), axis=0, keepdims=True)
        weight = isw_ref[:, cols]
        probs = jnp.where(valid, jnp.exp(log_probs), 0.0)
        grad = weight * (probs * jnp.sum(projected, axis=0, keepdims=True) - projected)
        grad16 = grad.astype(BF16)
        for a in range(ACT):
            glt[SLOT * a : SLOT * (a + 1), cols] = jnp.where(action == a, grad, 0.0).astype(BF16)
        ce_ref[:, cols] = cross
        return loss + weight * cross, jnp.maximum(top, cross)

    loss_row, top_row = lax.fori_loop(
        0, ROWS // 256, head, (jnp.zeros((1, 256), F32), jnp.full((1, 256), -jnp.inf, F32))
    )

    group = 6
    for g in range(ACT // group):
        rows = group * SLOT
        gl = glt[g * rows : (g + 1) * rows, :]
        gw2 = lax.dot_general(gl, hid[...], (((1,), (0,)), ((), ())), preferred_element_type=F32)
        for i in range(group):
            a = g * group + i
            part_ref[ATOM * a : ATOM * (a + 1), :] = gw2[SLOT * i : SLOT * i + ATOM, :]
    part_ref[HEADS:W1_AT, :] = jnp.zeros((W1_AT - HEADS, HID), F32)

    pl.semaphore_wait(barrier, len(near))
    waves, row, at = [], 0, 0
    for i, sizes in enumerate(WAVES):
        waves.append(Wave(i, sizes, row, me, core, send_sem, recv_sem, part_ref, tot, buffers[8 * i : 8 * (i + 1)]))
        row += 2 * sum(sizes)
    assert row == TOTAL_ROWS
    wave0, wave1, wave2 = waves
    wave0.swap()

    for a in range(ACT):
        ga = glt[SLOT * a : SLOT * (a + 1), :].astype(F32)
        gb2[ATOM * a : ATOM * (a + 1), :] = jnp.broadcast_to(jnp.sum(ga, axis=1, keepdims=True), (SLOT, 128))[:ATOM]
    gb2[HEADS:, :] = jnp.zeros((1024 - HEADS, 128), F32)
    gb2_row = gb2[...].T[0:1, :]

    def back(t, gb1):
        cols = pl.ds(pl.multiple_of(t * 256, 256), 256)
        gh = lax.dot_general(glt[:, cols], w2p[...], (((0,), (0,)), ((), ())), preferred_element_type=F32)
        g16 = jnp.where(hid[cols, :].astype(F32) > 0.0, gh, 0.0).astype(BF16)
        gp[cols, :] = g16
        return gb1 + jnp.sum(g16.astype(F32), axis=0, keepdims=True)

    gb1 = lax.fori_loop(0, ROWS // 256, back, jnp.zeros((1, HID), F32))

    lane = lax.broadcasted_iota(jnp.int32, (1, HID), 1)
    top = jnp.max(top_row)
    loss = jnp.sum(loss_row)
    part_ref[B1_AT:, :] = jnp.concatenate(
        [
            gb1,
            gb2_row[:, :HID],
            gb2_row[:, HID:],
            jnp.where(lane == me, top, 0.0),
            jnp.where(lane == 0, loss, 0.0),
            jnp.zeros((TOTAL_ROWS - LOSS_AT - 1, HID), F32),
        ],
        axis=0,
    )

    def grad_w1(wave, half, tiles, size):
        low = wave.row + half * wave.half
        start = jnp.maximum(low - W1_AT, 0)
        span = jnp.minimum(low + wave.half - W1_AT, FEAT) - start

        def tile(i, carry):
            at = start + jnp.minimum(i * size, span - size)
            rows = pl.ds(pl.multiple_of(at, 16), size)
            out = pl.ds(pl.multiple_of(at + W1_AT, 16), size)
            part_ref[out, :] = jnp.dot(feat[rows, :], gp[...], preferred_element_type=F32)
            return carry

        lax.fori_loop(0, tiles, tile, 0)

    steps = [wave.steps() for wave in waves]

    def go(text):
        for digit in text:
            next(steps[int(digit)])

    go("0")
    grad_w1(wave1, 1 - core, 3, 256)
    wave1.swap()
    grad_w1(wave1, core, 3, 256)
    grad_w1(wave2, 1 - core, 4, 224)
    wave2.swap()
    go("1")
    grad_w1(wave2, core, 4, 224)
    go(SCHEDULE)
    for wave in waves:
        wave.drain()


def finish_kernel(
    tot, ce, w1_out, b1_out, w2_out, b2_out, loss_out, prio, w2_copy, sems,
):
    first = pltpu.make_async_copy(tot.at[W1_AT:B1_AT, :], w1_out, sems.at[0])
    first.start()
    w2_copy[...] = tot[:HEADS, :]
    second = pltpu.make_async_copy(w2_copy, w2_out, sems.at[1])
    second.start()
    b1_out[...] = tot[B1_AT : B1_AT + 1, :]
    b2_out[...] = jnp.concatenate([tot[B2_AT : B2_AT + 1, :], tot[B2_AT + 1 : B2_AT + 2, :]], axis=1)[:, :HEADS]
    loss_out[...] = tot[LOSS_AT : LOSS_AT + 1, 0:1] * (1.0 / (ROWS * 128))
    top = jnp.max(tot[TOP_AT : TOP_AT + 1, 0:128])
    prio[...] = ce[...] / jnp.maximum(top, 1.0)
    first.wait()
    second.wait()


SCHEDULE = "0201021012012012012012120120122012"


RECEIVES = 21
LO, HI, ALL = slice(0, HID // 2), slice(HID // 2, HID), slice(0, HID)
ORDER = (2, 1, 3, 0)


def rows_at(start, size):
    return pl.ds(pl.multiple_of(start, 8), size)


def lanes_at(p):
    return pl.ds(pl.multiple_of(p * 128, 128), 128)


def ring(me, axis):
    stride = 32 - 33 * axis + 9 * axis * axis
    at = (me // stride) % 4
    return at, [me + stride * ((at + d) % 4 - at) for d in range(4)]


class Wave:
    def __init__(self, index, sizes, row, me, core, send_sem, recv_sem, part, tot, buffers):
        self.row, self.half, self.part, self.tot = row, sum(sizes), part, tot
        self.work, self.plus_a, self.minus_a, self.one_a, self.plus_b, self.minus_b, self.one_b, self.piece = buffers
        self.sizes = sizes
        self.first = [sum(sizes[:s]) for s in range(3)]
        self.base = row + core * self.half
        self.other = row + (1 - core) * self.half
        self.sibling = me + 1 - 2 * core
        self.mine = [[ring(me, (s + k + core) % 3) for k in range(3)] for s in range(3)]
        self.theirs = [ring(me, (s + 1 - core) % 3)[0] for s in range(3)]
        self.send_sem = send_sem.at[index]
        self.recv_sems = [recv_sem.at[index, i] for i in range(RECEIVES)]
        self.sent = 0

    def take(self):
        return self.recv_sems.pop(0)

    def send(self, src, dst, device, recv_sem):
        self.sent += src.shape[0] * src.shape[1]
        pltpu.make_async_remote_copy(
            src_ref=src, dst_ref=dst, send_sem=self.send_sem, recv_sem=recv_sem,
            device_id=(device,), device_id_type=MESH,
        ).start()

    def wait(self, sem, rows, lanes):
        ref = self.part.at[0:rows, 0:lanes]
        pltpu.make_async_copy(ref, ref, sem).wait()

    def drain(self):
        tiles = self.sent // 1024
        self.wait(self.send_sem, tiles // 4 * 8, HID)
        if tiles % 4:
            self.wait(self.send_sem, 8, tiles % 4 * 128)

    def swap(self):
        self.swapped = {d: self.take() for d in ORDER}
        for d in ORDER:
            for s in range(3):
                q = self.sizes[s] // 4
                at = (self.theirs[s] + d) % 4 * q + self.first[s]
                self.send(
                    self.part.at[rows_at(self.other + at, q), :], self.work.at[rows_at(at, q), :], self.sibling,
                    self.swapped[d],
                )

    def scatter(self, k, blocks, sizes, plus, minus, one, first_stage):
        send, work = self.send, self.work
        up, down, rest = self.take(), self.take(), self.take()
        quarter = {}
        for d in ORDER:
            if first_stage:
                self.wait(self.swapped[d], sum(sizes), HID)
            for s in range(3):
                at, ahead = self.mine[s][k]
                q = sizes[s]
                local = blocks[s] + (at + d) % 4 * q
                rows = rows_at(local, q)
                quarter[s, d] = rows
                if first_stage:
                    work[rows, :] = work[rows, :] + self.part[rows_at(self.base + local, q), :]
                here = pl.ds(0, q)
                if d == 2:
                    send(work.at[rows, LO], one.at[s, here, LO], ahead[1], up)
                    send(work.at[rows, HI], one.at[s, here, HI], ahead[3], down)
                elif d == 1:
                    send(work.at[rows, HI], plus.at[s, here, HI], ahead[1], rest)
                elif d == 3:
                    send(work.at[rows, LO], minus.at[s, here, LO], ahead[3], rest)
        yield
        for name, d, lanes, target, step in ((up, 1, LO, plus, 1), (down, 3, HI, minus, 3)):
            self.wait(name, sum(sizes), HID // 2)
            for s in range(3):
                rows, here = quarter[s, d], pl.ds(0, sizes[s])
                work[rows, lanes] = work[rows, lanes] + one[s, here, lanes]
                send(work.at[rows, lanes], target.at[s, here, lanes], self.mine[s][k][1][step], rest)
        yield
        self.wait(rest, 2 * sum(sizes), HID)
        for s in range(3):
            rows, here = quarter[s, 0], pl.ds(0, sizes[s])
            work[rows, :] = work[rows, :] + (plus[s, here, :] + minus[s, here, :])

    def gather(self, k, blocks, sizes, pair):
        up, down, rest, far = self.take(), self.take(), self.take(), self.take()
        both = self.take() if pair else None

        def put(s, d, lanes, device, sem):
            start = self.base + blocks[s] + (self.mine[s][k][0] + d) % 4 * sizes[s]
            ref = self.tot.at[rows_at(start, sizes[s]), lanes]
            self.send(ref, ref, device, sem)

        def to_sibling(*quarters):
            if pair:
                for s in range(3):
                    for d in quarters:
                        put(s, d, ALL, self.sibling, both)

        for lanes, step, sem in ((LO, 1, up), (HI, 3, down), (HI, 1, rest), (LO, 3, rest)):
            for s in range(3):
                put(s, 0, lanes, self.mine[s][k][1][step], sem)
        to_sibling(0)
        yield
        for sem, d, lanes, step in ((up, 3, LO, 1), (down, 1, HI, 3)):
            self.wait(sem, sum(sizes), HID // 2)
            for s in range(3):
                put(s, d, lanes, self.mine[s][k][1][step], far)
        yield
        self.wait(rest, sum(sizes), HID)
        to_sibling(3, 1)
        self.wait(far, sum(sizes), HID)
        to_sibling(2)
        if pair:
            yield
            self.wait(both, self.half, HID)

    def steps(self):
        size_a = [size // 4 for size in self.sizes]
        size_b = [size // 16 for size in self.sizes]
        block_a = self.first
        yield from self.scatter(0, block_a, size_a, self.plus_a, self.minus_a, self.one_a, True)
        block_b = [block_a[s] + self.mine[s][0][0] * size_a[s] for s in range(3)]
        yield from self.scatter(1, block_b, size_b, self.plus_b, self.minus_b, self.one_b, False)
        block_c = [block_b[s] + self.mine[s][1][0] * size_b[s] for s in range(3)]

        piece, work, tot = self.piece, self.work, self.tot
        last, final = self.take(), self.take()
        for d in (2, 1, 3):
            for s in range(3):
                at, ahead = self.mine[s][2]
                self.send(
                    work.at[rows_at(block_c[s], size_b[s]), lanes_at((at + d) % 4)],
                    piece.at[s, d - 1, pl.ds(0, size_b[s]), :], ahead[d], last,
                )
        yield
        self.wait(last, 3 * sum(size_b), 128)
        for s in range(3):
            at, ahead = self.mine[s][2]
            here = pl.ds(0, size_b[s])
            got = work[rows_at(block_c[s], size_b[s]), lanes_at(at)] + (piece[s, 0, here, :] + piece[s, 2, here, :])
            rows = rows_at(self.base + block_c[s], size_b[s])
            tot[rows, lanes_at(at)] = got + piece[s, 1, here, :]
            for d in (2, 1, 3):
                ref = tot.at[rows, lanes_at(at)]
                self.send(ref, ref, ahead[d], final)
        yield
        self.wait(final, 3 * sum(size_b), 128)
        yield from self.gather(1, block_b, size_b, False)
        yield from self.gather(0, block_a, size_a, True)
        yield


def wave_buffers(sizes):
    q, half = max(sizes) // 4, sum(sizes)
    return [
        pltpu.VMEM((half, HID), F32),
        pltpu.VMEM((3, q, HID), F32),
        pltpu.VMEM((3, q, HID), F32),
        pltpu.VMEM((3, q, HID), F32),
        pltpu.VMEM((3, q // 4, HID), F32),
        pltpu.VMEM((3, q // 4, HID), F32),
        pltpu.VMEM((3, q // 4, HID), F32),
        pltpu.VMEM((3, 3, q // 4, 128), F32),
    ]


def in_hbm(x):
    return pltpu.with_memory_space_constraint(x, pltpu.HBM)


def main(*args):
    hbm = pl.BlockSpec(memory_space=pltpu.HBM)
    vm = pl.BlockSpec(memory_space=pltpu.VMEM)
    buffers = []
    for sizes in WAVES:
        buffers += wave_buffers(sizes)
    return pl.pallas_call(
        main_kernel,
        name="gradients_and_sum",
        in_specs=[hbm] * 11,
        out_specs=[vm, vm],
        out_shape=[pltpu.VMEM((TOTAL_ROWS, HID), F32), pltpu.VMEM((1, ROWS), F32)],
        scratch_shapes=[
            pltpu.VMEM((FEAT, ROWS), BF16),
            pltpu.VMEM((FEAT, HID), BF16),
            pltpu.VMEM((1, HID), F32),
            pltpu.VMEM((HEADS, HID), BF16),
            pltpu.VMEM((1, HEADS), F32),
            pltpu.VMEM((1, ROWS), jnp.int32),
            pltpu.VMEM((ACT, ATOM, ROWS), F32),
            pltpu.VMEM((1, ROWS), jnp.int32),
            pltpu.VMEM((ATOM, ROWS), jnp.int32),
            pltpu.VMEM((ATOM, ROWS), F32),
            pltpu.VMEM((1, ROWS), F32),
            pltpu.VMEM((HEADS, HID), F32),
            pltpu.VMEM((HEAD, HID), BF16),
            pltpu.VMEM((1088, 128), F32),
            pltpu.VMEM((ATOM, 128), F32),
            pltpu.VMEM((ATOM, 128), F32),
            pltpu.VMEM((SLOT, ROWS), F32),
            pltpu.VMEM((ROWS, HID), BF16),
            pltpu.VMEM((HEAD, ROWS), BF16),
            pltpu.VMEM((ROWS, HID), BF16),
            pltpu.VMEM((1024, 128), F32),
            pltpu.VMEM((TOTAL_ROWS, HID), F32),
            pltpu.SemaphoreType.DMA((11,)),
            pltpu.SemaphoreType.DMA((len(WAVES),)),
            pltpu.SemaphoreType.DMA((len(WAVES), RECEIVES)),
            *buffers,
        ],
        compiler_params=pltpu.CompilerParams(
            vmem_limit_bytes=54 * 1024 * 1024, collective_id=0, has_side_effects=True
        ),
    )(*[in_hbm(x) for x in args])


def finish(tot, ce):
    hbm = pl.BlockSpec(memory_space=pltpu.HBM)
    vm = pl.BlockSpec(memory_space=pltpu.VMEM)
    return pl.pallas_call(
        finish_kernel,
        name="finish",
        in_specs=[vm, vm],
        out_specs=[hbm, vm, hbm, vm, vm, vm],
        out_shape=[
            jax.ShapeDtypeStruct((FEAT, HID), F32),
            jax.ShapeDtypeStruct((1, HID), F32),
            jax.ShapeDtypeStruct((HEADS, HID), F32),
            jax.ShapeDtypeStruct((1, HEADS), F32),
            jax.ShapeDtypeStruct((1, 1), F32),
            jax.ShapeDtypeStruct((1, ROWS), F32),
        ],
        scratch_shapes=[pltpu.VMEM((HEADS, HID), F32), pltpu.SemaphoreType.DMA((2,))],
        compiler_params=pltpu.CompilerParams(vmem_limit_bytes=8 * 1024 * 1024),
    )(tot, ce)


def on_device(features, w_one, b_one, w_two, b_two, action, target_probs, next_action, lower_idx, upper_frac, is_weight):
    tot, ce = main(
        features.T, w_one.T, b_one[None, :], w_two.T, b_two[None, :], action[None, :],
        target_probs.transpose(1, 2, 0), next_action[None, :], lower_idx.T, upper_frac.T, is_weight[None, :],
    )
    gw1, gb1, gw2, gb2, loss, prio = finish(tot, ce)
    return gw1.T, gb1[0], gw2.T, gb2[0], loss[0, 0], prio[0]


def solution(mesh):
    in_specs = (
        P("dp", None), P(), P(), P(), P(), P("dp"), P("dp", None, None), P("dp"), P("dp", None), P("dp", None), P("dp"),
    )
    out_specs = (P(), P(), P(), P(), P(), P("dp"))
    return jax.shard_map(on_device, mesh=mesh, in_specs=in_specs, out_specs=out_specs, check_vma=False)
```

```python
import functools

import jax
import jax.numpy as jnp
from jax import lax
from jax.experimental import pallas as pl
from jax.experimental.pallas import tpu as pltpu
from jax.sharding import PartitionSpec as P

MESH = pl.DeviceIdType.MESH
F32, BF16 = jnp.float32, jnp.bfloat16

FEAT, HID, ACT, ATOM, ROWS = 3136, 512, 18, 51, 1024
SLOT = 64
HEAD = ACT * SLOT
HEADS = ACT * ATOM

W1_AT = 928
B1_AT = W1_AT + FEAT
B2_AT = B1_AT + 1
TOP_AT = B2_AT + 2
LOSS_AT = TOP_AT + 1
TOTAL_ROWS = 4096
WAVES = (
    ((128, 128, 128), None),
    ((256, 256, 128), (3, 224)),
    ((256, 128, 256), (3, 224)),
    ((128, 128, 128), (2, 192)),
)
PLAN = "0aA0b1Bc02C12031230123102310321320312031233021"


def main_kernel(
    feat_hbm, w1_hbm, b1_hbm, w2_hbm, b2_hbm, act_hbm, tp_hbm, nact_hbm, low_hbm, frac_hbm, isw_hbm,
    tot, ce_ref,
    feat, w1, b1_ref, w2raw, b2_ref, act_ref, tp, nact_ref, low_ref, frac_ref, isw_ref,
    w2f, w2p, b2col, mlow, mhigh, proj, hid, glt, gp, gb2, part_ref, sems, send_sem, recv_sem, *buffers,
):
    me = lax.axis_index("dp")
    core = me % 2
    sibling = me + 1 - 2 * core
    pairs = [
        (w2_hbm, w2raw), (b2_hbm, b2_ref), (nact_hbm, nact_ref), (low_hbm, low_ref), (frac_hbm, frac_ref),
        (tp_hbm, tp), (w1_hbm, w1), (b1_hbm, b1_ref), (feat_hbm, feat), (act_hbm, act_ref), (isw_hbm, isw_ref),
    ]
    copies = [pltpu.make_async_copy(src, dst, sems.at[i]) for i, (src, dst) in enumerate(pairs)]
    for copy in copies:
        copy.start()
    near = [sibling]
    for axis in range(3):
        near += ring(me, axis)[1][1:]
    barrier = pltpu.get_barrier_semaphore()
    for device in near:
        pl.semaphore_signal(barrier, inc=1, device_id=(device,), device_id_type=MESH)

    copies[0].wait()
    copies[1].wait()
    w2f[...] = w2raw[...].astype(F32)
    wrow = lax.broadcasted_iota(jnp.int32, (SLOT, HID), 0)
    for a in range(ACT):
        if a < ACT - 1:
            block = w2f[ATOM * a : ATOM * a + SLOT, :]
        else:
            block = jnp.concatenate([w2f[ATOM * a : HEADS, :], jnp.zeros((SLOT - ATOM, HID), F32)], axis=0)
        w2p[SLOT * a : SLOT * (a + 1), :] = jnp.where(wrow < ATOM, block, 0.0).astype(BF16)
    b2row = jnp.concatenate([b2_ref[...], jnp.zeros((1, 1024 - HEADS), F32)], axis=1)
    b2col[0:1024, :] = jnp.broadcast_to(b2row, (128, 1024)).T
    b2col[1024:, :] = jnp.zeros((64, 128), F32)

    for copy in copies[2:6]:
        copy.wait()
    atom_row = lax.broadcasted_iota(jnp.int32, (SLOT, 128), 0)

    def project(t, carry):
        lanes = pl.ds(pl.multiple_of(t * 128, 128), 128)
        nact = nact_ref[:, lanes]
        probs = jnp.zeros((ATOM, 128), F32)
        for a in range(ACT):
            probs = jnp.where(nact == a, tp[a, :, lanes], probs)
        frac = frac_ref[:, lanes]
        mlow[...] = probs * (1.0 - frac)
        mhigh[...] = probs * frac
        low_sum = jnp.zeros((SLOT, 128), F32)
        high_sum = jnp.zeros((SLOT, 128), F32)
        for j in range(ATOM):
            hot = low_ref[pl.ds(j, 1), lanes] == atom_row
            low_sum = low_sum + jnp.where(hot, mlow[pl.ds(j, 1), :], 0.0)
            high_sum = high_sum + jnp.where(hot, mhigh[pl.ds(j, 1), :], 0.0)
        high_sum = jnp.where(atom_row == 0, 0.0, pltpu.roll(high_sum, 1, 0))
        proj[:, lanes] = low_sum + high_sum
        return carry

    lax.fori_loop(0, ROWS // 128, project, 0)

    for copy in copies[6:]:
        copy.wait()

    def forward(t, carry):
        cols = pl.ds(pl.multiple_of(t * 256, 256), 256)
        pre = lax.dot_general(feat[:, cols], w1[...], (((0,), (0,)), ((), ())), preferred_element_type=F32)
        hid[cols, :] = jnp.maximum(pre + b1_ref[...], 0.0).astype(BF16)
        return carry

    lax.fori_loop(0, ROWS // 256, forward, 0)

    valid = lax.broadcasted_iota(jnp.int32, (SLOT, 256), 0) < ATOM

    def head(t, carry):
        loss, top = carry
        cols = pl.ds(pl.multiple_of(t * 256, 256), 256)
        logits = lax.dot_general(w2p[...], hid[cols, :], (((1,), (1,)), ((), ())), preferred_element_type=F32)
        action = act_ref[:, cols]
        chosen = jnp.zeros((SLOT, 256), F32)
        for a in range(ACT):
            bias = b2col[ATOM * a : ATOM * a + SLOT, :]
            biased = logits[SLOT * a : SLOT * (a + 1), :] + jnp.concatenate([bias, bias], axis=1)
            chosen = jnp.where(action == a, biased, chosen)
        chosen = jnp.where(valid, chosen, -1e30)
        shifted = chosen - jnp.max(chosen, axis=0, keepdims=True)
        expd = jnp.where(valid, jnp.exp(shifted), 0.0)
        log_probs = shifted - jnp.log(jnp.sum(expd, axis=0, keepdims=True))
        projected = proj[:, cols]
        cross = -jnp.sum(jnp.where(valid, projected * log_probs, 0.0), axis=0, keepdims=True)
        weight = isw_ref[:, cols]
        probs = jnp.where(valid, jnp.exp(log_probs), 0.0)
        grad = weight * (probs * jnp.sum(projected, axis=0, keepdims=True) - projected)
        grad16 = grad.astype(BF16)
        for a in range(ACT):
            glt[SLOT * a : SLOT * (a + 1), cols] = jnp.where(action == a, grad, 0.0).astype(BF16)
        ce_ref[:, cols] = cross
        return loss + weight * cross, jnp.maximum(top, cross)

    loss_row, top_row = lax.fori_loop(
        0, ROWS // 256, head, (jnp.zeros((1, 256), F32), jnp.full((1, 256), -jnp.inf, F32))
    )

    group = 6
    for g in range(ACT // group):
        rows = group * SLOT
        gl = glt[g * rows : (g + 1) * rows, :]
        gw2 = lax.dot_general(gl, hid[...], (((1,), (0,)), ((), ())), preferred_element_type=F32)
        for i in range(group):
            a = g * group + i
            part_ref[ATOM * a : ATOM * (a + 1), :] = gw2[SLOT * i : SLOT * i + ATOM, :]
    part_ref[HEADS:W1_AT, :] = jnp.zeros((W1_AT - HEADS, HID), F32)

    pl.semaphore_wait(barrier, len(near))
    waves, row, at = [], 0, 0
    for i, (sizes, _) in enumerate(WAVES):
        waves.append(Wave(i, sizes, row, me, core, send_sem, recv_sem, part_ref, tot, buffers[6 * i : 6 * (i + 1)]))
        row += 2 * sum(sizes)
    assert row == TOTAL_ROWS
    waves[0].swap()

    for a in range(ACT):
        ga = glt[SLOT * a : SLOT * (a + 1), :].astype(F32)
        gb2[ATOM * a : ATOM * (a + 1), :] = jnp.broadcast_to(jnp.sum(ga, axis=1, keepdims=True), (SLOT, 128))[:ATOM]
    gb2[HEADS:, :] = jnp.zeros((1024 - HEADS, 128), F32)
    gb2_row = gb2[...].T[0:1, :]

    def back(t, gb1):
        cols = pl.ds(pl.multiple_of(t * 256, 256), 256)
        gh = lax.dot_general(glt[:, cols], w2p[...], (((0,), (0,)), ((), ())), preferred_element_type=F32)
        g16 = jnp.where(hid[cols, :].astype(F32) > 0.0, gh, 0.0).astype(BF16)
        gp[cols, :] = g16
        return gb1 + jnp.sum(g16.astype(F32), axis=0, keepdims=True)

    gb1 = lax.fori_loop(0, ROWS // 256, back, jnp.zeros((1, HID), F32))

    lane = lax.broadcasted_iota(jnp.int32, (1, HID), 1)
    top = jnp.max(top_row)
    loss = jnp.sum(loss_row)
    part_ref[B1_AT:, :] = jnp.concatenate(
        [
            gb1,
            gb2_row[:, :HID],
            gb2_row[:, HID:],
            jnp.where(lane == me, top, 0.0),
            jnp.where(lane == 0, loss, 0.0),
            jnp.zeros((TOTAL_ROWS - LOSS_AT - 1, HID), F32),
        ],
        axis=0,
    )

    def grad_w1(wave, half, tiles, size):
        low = wave.row + half * wave.half
        start = jnp.maximum(low - W1_AT, 0)
        span = jnp.minimum(low + wave.half - W1_AT, FEAT) - start

        def tile(i, carry):
            at = start + jnp.minimum(i * size, span - size)
            rows = pl.ds(pl.multiple_of(at, 16), size)
            out = pl.ds(pl.multiple_of(at + W1_AT, 16), size)
            part_ref[out, :] = jnp.dot(feat[rows, :], gp[...], preferred_element_type=F32)
            return carry

        lax.fori_loop(0, tiles, tile, 0)

    steps = [wave.steps() for wave in waves]

    for token in PLAN:
        i = "0ABCD".find(token.upper())
        if i > 0:
            other = token.islower()
            grad_w1(waves[i], 1 - core if other else core, *WAVES[i][1])
            if other:
                waves[i].swap()
        else:
            next(steps[int(token)])
    for wave in waves:
        wave.drain()


def finish_kernel(
    tot, ce, w1_out, b1_out, w2_out, b2_out, loss_out, prio, w2_copy, sems,
):
    copies = []
    for i in range(7):
        rows = pl.ds(448 * i, 448)
        copies.append(pltpu.make_async_copy(tot.at[pl.ds(W1_AT + 448 * i, 448), :], w1_out.at[rows, :], sems.at[i]))
        copies[i].start()
    w2_copy[...] = tot[:HEADS, :]
    copies.append(pltpu.make_async_copy(w2_copy, w2_out, sems.at[7]))
    copies[7].start()
    b1_out[...] = tot[B1_AT : B1_AT + 1, :]
    b2_out[...] = jnp.concatenate([tot[B2_AT : B2_AT + 1, :], tot[B2_AT + 1 : B2_AT + 2, :]], axis=1)[:, :HEADS]
    loss_out[...] = tot[LOSS_AT : LOSS_AT + 1, 0:1] * (1.0 / (ROWS * 128))
    top = jnp.max(tot[TOP_AT : TOP_AT + 1, 0:128])
    prio[...] = ce[...] / jnp.maximum(top, 1.0)
    for copy in copies:
        copy.wait()


RECEIVES = 16
LO, HI, ALL = slice(0, HID // 2), slice(HID // 2, HID), slice(0, HID)
ORDER = (2, 1, 3, 0)


def rows_at(start, size):
    return pl.ds(pl.multiple_of(start, 8), size)


def lanes_at(p):
    return pl.ds(pl.multiple_of(p * 128, 128), 128)


def ring(me, axis):
    stride = 32 - 33 * axis + 9 * axis * axis
    at = (me // stride) % 4
    return at, [me + stride * ((at + d) % 4 - at) for d in range(4)]


class Wave:
    def __init__(self, index, sizes, row, me, core, send_sem, recv_sem, part, tot, buffers):
        self.row, self.half, self.part, self.tot = row, sum(sizes), part, tot
        self.work, self.plus, self.minus, self.one, self.whole, self.piece = buffers
        self.sizes = sizes
        self.first = [sum(sizes[:s]) for s in range(3)]
        self.base = row + core * self.half
        self.other = row + (1 - core) * self.half
        self.sibling = me + 1 - 2 * core
        self.mine = [[ring(me, (s + k + core) % 3) for k in range(3)] for s in range(3)]
        self.theirs = [ring(me, (s + 1 - core) % 3)[0] for s in range(3)]
        self.send_sem = send_sem.at[index]
        self.recv_sems = [recv_sem.at[index, i] for i in range(RECEIVES)]
        self.sent = 0

    def take(self):
        return self.recv_sems.pop(0)

    def send(self, src, dst, device, recv_sem):
        self.sent += src.shape[0] * src.shape[1]
        pltpu.make_async_remote_copy(
            src_ref=src, dst_ref=dst, send_sem=self.send_sem, recv_sem=recv_sem,
            device_id=(device,), device_id_type=MESH,
        ).start()

    def wait(self, sem, rows, lanes):
        ref = self.part.at[0:rows, 0:lanes]
        pltpu.make_async_copy(ref, ref, sem).wait()

    def drain(self):
        tiles = self.sent // 1024
        self.wait(self.send_sem, tiles // 4 * 8, HID)
        if tiles % 4:
            self.wait(self.send_sem, 8, tiles % 4 * 128)

    def swap(self):
        self.swapped = {d: self.take() for d in ORDER}
        for d in ORDER:
            for s in range(3):
                q = self.sizes[s] // 4
                at = (self.theirs[s] + d) % 4 * q + self.first[s]
                self.send(
                    self.part.at[rows_at(self.other + at, q), :], self.work.at[rows_at(at, q), :], self.sibling,
                    self.swapped[d],
                )

    def scatter(self, blocks, sizes):
        k, send, work, plus, minus, one = 0, self.send, self.work, self.plus, self.minus, self.one
        up, down, rest = self.take(), self.take(), self.take()
        quarter = {}
        for d in ORDER:
            self.wait(self.swapped[d], sum(sizes), HID)
            for s in range(3):
                at, ahead = self.mine[s][k]
                q = sizes[s]
                local = blocks[s] + (at + d) % 4 * q
                rows = rows_at(local, q)
                quarter[s, d] = rows
                work[rows, :] = work[rows, :] + self.part[rows_at(self.base + local, q), :]
                here = pl.ds(0, q)
                if d == 2:
                    send(work.at[rows, LO], one.at[s, here, LO], ahead[1], up)
                    send(work.at[rows, HI], one.at[s, here, HI], ahead[3], down)
                elif d == 1:
                    send(work.at[rows, HI], plus.at[s, here, HI], ahead[1], rest)
                elif d == 3:
                    send(work.at[rows, LO], minus.at[s, here, LO], ahead[3], rest)
        yield
        for name, d, lanes, target, step in ((up, 1, LO, plus, 1), (down, 3, HI, minus, 3)):
            self.wait(name, sum(sizes), HID // 2)
            for s in range(3):
                rows, here = quarter[s, d], pl.ds(0, sizes[s])
                work[rows, lanes] = work[rows, lanes] + one[s, here, lanes]
                send(work.at[rows, lanes], target.at[s, here, lanes], self.mine[s][k][1][step], rest)
        yield
        self.wait(rest, 2 * sum(sizes), HID)
        for s in range(3):
            rows, here = quarter[s, 0], pl.ds(0, sizes[s])
            work[rows, :] = work[rows, :] + (plus[s, here, :] + minus[s, here, :])

    def scatter_straight(self, blocks, sizes):
        whole, work, sem = self.whole, self.work, self.take()
        for d in (2, 1, 3):
            for s in range(3):
                at, ahead = self.mine[s][1]
                rows = rows_at(blocks[s] + (at + d) % 4 * sizes[s], sizes[s])
                self.send(work.at[rows, ALL], whole.at[s, d - 1, pl.ds(0, sizes[s]), :], ahead[d], sem)
        yield
        self.wait(sem, 3 * sum(sizes), HID)
        for s in range(3):
            rows, here = rows_at(blocks[s] + self.mine[s][1][0] * sizes[s], sizes[s]), pl.ds(0, sizes[s])
            work[rows, :] = (work[rows, :] + whole[s, 1, here, :]) + (whole[s, 0, here, :] + whole[s, 2, here, :])

    def put(self, k, blocks, sizes, s, d, lanes, device, sem):
        start = self.base + blocks[s] + (self.mine[s][k][0] + d) % 4 * sizes[s]
        ref = self.tot.at[rows_at(start, sizes[s]), lanes]
        self.send(ref, ref, device, sem)

    def gather_straight(self, blocks, sizes):
        sem = self.take()
        for d in (2, 1, 3):
            for s in range(3):
                self.put(1, blocks, sizes, s, 0, ALL, self.mine[s][1][1][d], sem)
        yield
        self.wait(sem, 3 * sum(sizes), HID)

    def gather(self, blocks, sizes):
        up, down, rest, far, both = self.take(), self.take(), self.take(), self.take(), self.take()
        put = functools.partial(self.put, 0, blocks, sizes)

        def to_sibling(*quarters):
            for s in range(3):
                for d in quarters:
                    put(s, d, ALL, self.sibling, both)

        for lanes, step, sem in ((LO, 1, up), (HI, 3, down), (HI, 1, rest), (LO, 3, rest)):
            for s in range(3):
                put(s, 0, lanes, self.mine[s][0][1][step], sem)
        to_sibling(0)
        yield
        for sem, d, lanes, step in ((up, 3, LO, 1), (down, 1, HI, 3)):
            self.wait(sem, sum(sizes), HID // 2)
            for s in range(3):
                put(s, d, lanes, self.mine[s][0][1][step], far)
        yield
        self.wait(rest, sum(sizes), HID)
        to_sibling(3, 1)
        self.wait(far, sum(sizes), HID)
        to_sibling(2)
        yield
        self.wait(both, self.half, HID)

    def steps(self):
        size_a = [size // 4 for size in self.sizes]
        size_b = [size // 16 for size in self.sizes]
        block_a = self.first
        yield from self.scatter(block_a, size_a)
        block_b = [block_a[s] + self.mine[s][0][0] * size_a[s] for s in range(3)]
        yield from self.scatter_straight(block_b, size_b)
        block_c = [block_b[s] + self.mine[s][1][0] * size_b[s] for s in range(3)]

        piece, work, tot = self.piece, self.work, self.tot
        last, final = self.take(), self.take()
        for d in (2, 1, 3):
            for s in range(3):
                at, ahead = self.mine[s][2]
                self.send(
                    work.at[rows_at(block_c[s], size_b[s]), lanes_at((at + d) % 4)],
                    piece.at[s, d - 1, pl.ds(0, size_b[s]), :], ahead[d], last,
                )
        yield
        self.wait(last, 3 * sum(size_b), 128)
        for s in range(3):
            at, ahead = self.mine[s][2]
            here = pl.ds(0, size_b[s])
            got = work[rows_at(block_c[s], size_b[s]), lanes_at(at)] + (piece[s, 0, here, :] + piece[s, 2, here, :])
            rows = rows_at(self.base + block_c[s], size_b[s])
            tot[rows, lanes_at(at)] = got + piece[s, 1, here, :]
            for d in (2, 1, 3):
                ref = tot.at[rows, lanes_at(at)]
                self.send(ref, ref, ahead[d], final)
        yield
        self.wait(final, 3 * sum(size_b), 128)
        yield from self.gather_straight(block_b, size_b)
        yield from self.gather(block_a, size_a)
        yield


def wave_buffers(sizes):
    q, half = max(sizes) // 4, sum(sizes)
    return [
        pltpu.VMEM((half, HID), F32),
        pltpu.VMEM((3, q, HID), F32),
        pltpu.VMEM((3, q, HID), F32),
        pltpu.VMEM((3, q, HID), F32),
        pltpu.VMEM((3, 3, q // 4, HID), F32),
        pltpu.VMEM((3, 3, q // 4, 128), F32),
    ]


def in_hbm(x):
    return pltpu.with_memory_space_constraint(x, pltpu.HBM)


def main(*args):
    hbm = pl.BlockSpec(memory_space=pltpu.HBM)
    vm = pl.BlockSpec(memory_space=pltpu.VMEM)
    buffers = []
    for sizes, _ in WAVES:
        buffers += wave_buffers(sizes)
    return pl.pallas_call(
        main_kernel,
        name="gradients_and_sum",
        in_specs=[hbm] * 11,
        out_specs=[vm, vm],
        out_shape=[pltpu.VMEM((TOTAL_ROWS, HID), F32), pltpu.VMEM((1, ROWS), F32)],
        scratch_shapes=[
            pltpu.VMEM((FEAT, ROWS), BF16),
            pltpu.VMEM((FEAT, HID), BF16),
            pltpu.VMEM((1, HID), F32),
            pltpu.VMEM((HEADS, HID), BF16),
            pltpu.VMEM((1, HEADS), F32),
            pltpu.VMEM((1, ROWS), jnp.int32),
            pltpu.VMEM((ACT, ATOM, ROWS), F32),
            pltpu.VMEM((1, ROWS), jnp.int32),
            pltpu.VMEM((ATOM, ROWS), jnp.int32),
            pltpu.VMEM((ATOM, ROWS), F32),
            pltpu.VMEM((1, ROWS), F32),
            pltpu.VMEM((HEADS, HID), F32),
            pltpu.VMEM((HEAD, HID), BF16),
            pltpu.VMEM((1088, 128), F32),
            pltpu.VMEM((ATOM, 128), F32),
            pltpu.VMEM((ATOM, 128), F32),
            pltpu.VMEM((SLOT, ROWS), F32),
            pltpu.VMEM((ROWS, HID), BF16),
            pltpu.VMEM((HEAD, ROWS), BF16),
            pltpu.VMEM((ROWS, HID), BF16),
            pltpu.VMEM((1024, 128), F32),
            pltpu.VMEM((TOTAL_ROWS, HID), F32),
            pltpu.SemaphoreType.DMA((11,)),
            pltpu.SemaphoreType.DMA((len(WAVES),)),
            pltpu.SemaphoreType.DMA((len(WAVES), RECEIVES)),
            *buffers,
        ],
        compiler_params=pltpu.CompilerParams(
            vmem_limit_bytes=54 * 1024 * 1024, collective_id=0, has_side_effects=True
        ),
    )(*[in_hbm(x) for x in args])


def finish(tot, ce):
    hbm = pl.BlockSpec(memory_space=pltpu.HBM)
    vm = pl.BlockSpec(memory_space=pltpu.VMEM)
    return pl.pallas_call(
        finish_kernel,
        name="finish",
        in_specs=[vm, vm],
        out_specs=[hbm, vm, hbm, vm, vm, vm],
        out_shape=[
            jax.ShapeDtypeStruct((FEAT, HID), F32),
            jax.ShapeDtypeStruct((1, HID), F32),
            jax.ShapeDtypeStruct((HEADS, HID), F32),
            jax.ShapeDtypeStruct((1, HEADS), F32),
            jax.ShapeDtypeStruct((1, 1), F32),
            jax.ShapeDtypeStruct((1, ROWS), F32),
        ],
        scratch_shapes=[pltpu.VMEM((HEADS, HID), F32), pltpu.SemaphoreType.DMA((8,))],
        compiler_params=pltpu.CompilerParams(vmem_limit_bytes=8 * 1024 * 1024),
    )(tot, ce)


def on_device(features, w_one, b_one, w_two, b_two, action, target_probs, next_action, lower_idx, upper_frac, is_weight):
    tot, ce = main(
        features.T, w_one.T, b_one[None, :], w_two.T, b_two[None, :], action[None, :],
        target_probs.transpose(1, 2, 0), next_action[None, :], lower_idx.T, upper_frac.T, is_weight[None, :],
    )
    gw1, gb1, gw2, gb2, loss, prio = finish(tot, ce)
    return gw1.T, gb1[0], gw2.T, gb2[0], loss[0, 0], prio[0]


def solution(mesh):
    in_specs = (
        P("dp", None), P(), P(), P(), P(), P("dp"), P("dp", None, None), P("dp"), P("dp", None), P("dp", None), P("dp"),
    )
    out_specs = (P(), P(), P(), P(), P(), P("dp"))
    return jax.shard_map(on_device, mesh=mesh, in_specs=in_specs, out_specs=out_specs, check_vma=False)
```

```python
import functools

import jax
import jax.numpy as jnp
from jax import lax
from jax.experimental import pallas as pl
from jax.experimental.pallas import tpu as pltpu
from jax.sharding import PartitionSpec as P

MESH = pl.DeviceIdType.MESH
F32, BF16 = jnp.float32, jnp.bfloat16

FEAT, HID, ACT, ATOM, ROWS = 3136, 512, 18, 51, 1024
SLOT = 64
HEAD = ACT * SLOT
HEADS = ACT * ATOM

W1_AT = 928
B1_AT = W1_AT + FEAT
B2_AT = B1_AT + 1
TOP_AT = B2_AT + 2
LOSS_AT = TOP_AT + 1
TOTAL_ROWS = 4096
WAVES = (
    ((128, 128, 128), None),
    ((256, 128, 128), (2, 256)),
    ((128, 256, 128), (2, 256)),
    ((256, 128, 256), (2, 320)),
)
PLAN = "0aAb1B02c1C03102310231203120312301231201320323"


def main_kernel(
    feat_hbm, w1_hbm, b1_hbm, w2_hbm, b2_hbm, act_hbm, tp_hbm, nact_hbm, low_hbm, frac_hbm, isw_hbm,
    tot, ce_ref,
    feat, w1, b1_ref, w2raw, b2_ref, act_ref, tp, nact_ref, low_ref, frac_ref, isw_ref,
    w2f, w2p, b2col, mlow, mhigh, proj, hid, glt, gp, gb2, part_ref, sems, send_sem, recv_sem, *buffers,
):
    me = lax.axis_index("dp")
    core = me % 2
    sibling = me + 1 - 2 * core
    left, right = slice(0, ROWS // 2), slice(ROWS // 2, ROWS)
    pairs = [
        (w2_hbm, w2raw), (b2_hbm, b2_ref), (nact_hbm, nact_ref), (low_hbm, low_ref), (frac_hbm, frac_ref),
        (tp_hbm, tp), (b1_hbm, b1_ref), (act_hbm, act_ref), (isw_hbm, isw_ref),
        (w1_hbm, w1), (feat_hbm.at[:, left], feat.at[:, left]), (feat_hbm.at[:, right], feat.at[:, right]),
    ]
    copies = [pltpu.make_async_copy(src, dst, sems.at[i]) for i, (src, dst) in enumerate(pairs)]
    for copy in copies[:9]:
        copy.start()
    near = [sibling]
    for axis in range(3):
        near += ring(me, axis)[1][1:]
    barrier = pltpu.get_barrier_semaphore()
    for device in near:
        pl.semaphore_signal(barrier, inc=1, device_id=(device,), device_id_type=MESH)

    copies[0].wait()
    for copy in copies[9:]:
        copy.start()
    copies[1].wait()
    w2f[...] = w2raw[...].astype(F32)
    wrow = lax.broadcasted_iota(jnp.int32, (SLOT, HID), 0)
    for a in range(ACT):
        if a < ACT - 1:
            block = w2f[ATOM * a : ATOM * a + SLOT, :]
        else:
            block = jnp.concatenate([w2f[ATOM * a : HEADS, :], jnp.zeros((SLOT - ATOM, HID), F32)], axis=0)
        w2p[SLOT * a : SLOT * (a + 1), :] = jnp.where(wrow < ATOM, block, 0.0).astype(BF16)
    b2row = jnp.concatenate([b2_ref[...], jnp.zeros((1, 1024 - HEADS), F32)], axis=1)
    b2col[0:1024, :] = jnp.broadcast_to(b2row, (128, 1024)).T
    b2col[1024:, :] = jnp.zeros((64, 128), F32)

    for copy in copies[2:6]:
        copy.wait()
    atom_row = lax.broadcasted_iota(jnp.int32, (56, 128), 0)
    proj[56:, :] = jnp.zeros((SLOT - 56, ROWS), F32)

    def project(t, carry):
        lanes = pl.ds(pl.multiple_of(t * 128, 128), 128)
        nact = nact_ref[:, lanes]
        probs = jnp.zeros((ATOM, 128), F32)
        for a in range(ACT):
            probs = jnp.where(nact == a, tp[a, :, lanes], probs)
        frac = frac_ref[:, lanes]
        mlow[...] = probs * (1.0 - frac)
        mhigh[...] = probs * frac
        low_sum = jnp.zeros((56, 128), F32)
        high_sum = jnp.zeros((56, 128), F32)
        for j in range(ATOM):
            hot = low_ref[pl.ds(j, 1), lanes] == atom_row
            low_sum = low_sum + jnp.where(hot, mlow[pl.ds(j, 1), :], 0.0)
            high_sum = high_sum + jnp.where(hot, mhigh[pl.ds(j, 1), :], 0.0)
        high_sum = jnp.where(atom_row == 0, 0.0, pltpu.roll(high_sum, 1, 0))
        proj[0:56, lanes] = low_sum + high_sum
        return carry

    lax.fori_loop(0, ROWS // 128, project, 0)

    for copy in copies[6:10]:
        copy.wait()

    for t in range(2):
        copies[10 + t].wait()
        cols = slice(512 * t, 512 * (t + 1))
        pre = lax.dot_general(feat[:, cols], w1[...], (((0,), (0,)), ((), ())), preferred_element_type=F32)
        hid[cols, :] = jnp.maximum(pre + b1_ref[...], 0.0).astype(BF16)

    valid = lax.broadcasted_iota(jnp.int32, (SLOT, 256), 0) < ATOM

    def head(t, carry):
        loss, top = carry
        cols = slice(256 * t, 256 * (t + 1))
        logits = lax.dot_general(w2p[...], hid[cols, :], (((1,), (1,)), ((), ())), preferred_element_type=F32)
        action = act_ref[:, cols]
        chosen = jnp.zeros((SLOT, 256), F32)
        for a in range(ACT):
            bias = b2col[ATOM * a : ATOM * a + SLOT, :]
            biased = logits[SLOT * a : SLOT * (a + 1), :] + jnp.concatenate([bias, bias], axis=1)
            chosen = jnp.where(action == a, biased, chosen)
        chosen = jnp.where(valid, chosen, -1e30)
        shifted = chosen - jnp.max(chosen, axis=0, keepdims=True)
        expd = jnp.where(valid, jnp.exp(shifted), 0.0)
        log_probs = shifted - jnp.log(jnp.sum(expd, axis=0, keepdims=True))
        projected = proj[:, cols]
        cross = -jnp.sum(jnp.where(valid, projected * log_probs, 0.0), axis=0, keepdims=True)
        weight = isw_ref[:, cols]
        probs = jnp.where(valid, jnp.exp(log_probs), 0.0)
        grad = weight * (probs * jnp.sum(projected, axis=0, keepdims=True) - projected)
        grad16 = grad.astype(BF16)
        for a in range(ACT):
            glt[SLOT * a : SLOT * (a + 1), cols] = jnp.where(action == a, grad, 0.0).astype(BF16)
        ce_ref[:, cols] = cross
        return loss + weight * cross, jnp.maximum(top, cross)

    carry = (jnp.zeros((1, 256), F32), jnp.full((1, 256), -jnp.inf, F32))
    for t in range(ROWS // 256):
        carry = head(t, carry)
    loss_row, top_row = carry

    group = 6
    for g in range(ACT // group):
        rows = group * SLOT
        gl = glt[g * rows : (g + 1) * rows, :]
        gw2 = lax.dot_general(gl, hid[...], (((1,), (0,)), ((), ())), preferred_element_type=F32)
        for i in range(group):
            a = g * group + i
            part_ref[ATOM * a : ATOM * (a + 1), :] = gw2[SLOT * i : SLOT * i + ATOM, :]
    part_ref[HEADS:W1_AT, :] = jnp.zeros((W1_AT - HEADS, HID), F32)

    pl.semaphore_wait(barrier, len(near))
    waves, row, at = [], 0, 0
    for i, (sizes, _) in enumerate(WAVES):
        waves.append(Wave(i, sizes, row, me, core, send_sem, recv_sem, part_ref, tot, buffers[6 * i : 6 * (i + 1)]))
        row += 2 * sum(sizes)
    assert row == TOTAL_ROWS
    waves[0].swap()

    for a in range(ACT):
        ga = glt[SLOT * a : SLOT * (a + 1), :].astype(F32)
        gb2[ATOM * a : ATOM * (a + 1), :] = jnp.broadcast_to(jnp.sum(ga, axis=1, keepdims=True), (SLOT, 128))[:ATOM]
    gb2[HEADS:, :] = jnp.zeros((1024 - HEADS, 128), F32)
    gb2_row = gb2[...].T[0:1, :]

    def back(t, gb1):
        cols = pl.ds(pl.multiple_of(t * 512, 512), 512)
        gh = lax.dot_general(glt[:, cols], w2p[...], (((0,), (0,)), ((), ())), preferred_element_type=F32)
        g16 = jnp.where(hid[cols, :].astype(F32) > 0.0, gh, 0.0).astype(BF16)
        gp[cols, :] = g16
        return gb1 + jnp.sum(g16.astype(F32), axis=0, keepdims=True)

    gb1 = lax.fori_loop(0, ROWS // 512, back, jnp.zeros((1, HID), F32))

    lane = lax.broadcasted_iota(jnp.int32, (1, HID), 1)
    top = jnp.max(top_row)
    loss = jnp.sum(loss_row)
    part_ref[B1_AT:, :] = jnp.concatenate(
        [
            gb1,
            gb2_row[:, :HID],
            gb2_row[:, HID:],
            jnp.where(lane == me, top, 0.0),
            jnp.where(lane == 0, loss, 0.0),
            jnp.zeros((TOTAL_ROWS - LOSS_AT - 1, HID), F32),
        ],
        axis=0,
    )

    def grad_w1(wave, half, tiles, size):
        low = wave.row + half * wave.half
        start = jnp.maximum(low - W1_AT, 0)
        span = jnp.minimum(low + wave.half - W1_AT, FEAT) - start

        def tile(i, carry):
            at = start + jnp.minimum(i * size, span - size)
            rows = pl.ds(pl.multiple_of(at, 16), size)
            out = pl.ds(pl.multiple_of(at + W1_AT, 16), size)
            part_ref[out, :] = jnp.dot(feat[rows, :], gp[...], preferred_element_type=F32)
            return carry

        lax.fori_loop(0, tiles, tile, 0)

    steps = [wave.steps() for wave in waves]

    for token in PLAN:
        i = "0ABCD".find(token.upper())
        if i > 0:
            other = token.islower()
            grad_w1(waves[i], 1 - core if other else core, *WAVES[i][1])
            if other:
                waves[i].swap()
        else:
            next(steps[int(token)])
    for wave in waves:
        wave.drain()


def finish_kernel(
    tot, ce, w1_out, b1_out, w2_out, b2_out, loss_out, prio_out, w2_copy, b1_copy, b2_copy, loss_copy, prio_copy, sems,
):
    copies = []

    def copy_out(src, dst):
        copies.append(pltpu.make_async_copy(src, dst, sems.at[len(copies)]))
        copies[-1].start()

    w2_copy[...] = tot[:HEADS, :]
    copy_out(w2_copy, w2_out)
    for i in range(4):
        copy_out(tot.at[pl.ds(W1_AT + 784 * i, 784), :], w1_out.at[pl.ds(784 * i, 784), :])
    b1_copy[...] = tot[B1_AT : B1_AT + 1, :]
    copy_out(b1_copy, b1_out)
    b2_copy[...] = jnp.concatenate([tot[B2_AT : B2_AT + 1, :], tot[B2_AT + 1 : B2_AT + 2, :]], axis=1)[:, :HEADS]
    copy_out(b2_copy, b2_out)
    loss_copy[...] = tot[LOSS_AT : LOSS_AT + 1, 0:1] * (1.0 / (ROWS * 128))
    copy_out(loss_copy, loss_out)
    top = jnp.max(tot[TOP_AT : TOP_AT + 1, 0:128])
    prio_copy[...] = ce[...] / jnp.maximum(top, 1.0)
    copy_out(prio_copy, prio_out)
    for copy in copies:
        copy.wait()


RECEIVES = 16
LO, HI, ALL = slice(0, HID // 2), slice(HID // 2, HID), slice(0, HID)
ORDER = (2, 1, 3, 0)


def rows_at(start, size):
    return pl.ds(pl.multiple_of(start, 8), size)


def lanes_at(p):
    return pl.ds(pl.multiple_of(p * 128, 128), 128)


def ring(me, axis):
    stride = 32 - 33 * axis + 9 * axis * axis
    at = (me // stride) % 4
    return at, [me + stride * ((at + d) % 4 - at) for d in range(4)]


class Wave:
    def __init__(self, index, sizes, row, me, core, send_sem, recv_sem, part, tot, buffers):
        self.row, self.half, self.part, self.tot = row, sum(sizes), part, tot
        self.work, self.plus, self.minus, self.one, self.whole, self.piece = buffers
        self.sizes = sizes
        self.first = [sum(sizes[:s]) for s in range(3)]
        self.base = row + core * self.half
        self.other = row + (1 - core) * self.half
        self.sibling = me + 1 - 2 * core
        self.mine = [[ring(me, (s + k + core) % 3) for k in range(3)] for s in range(3)]
        self.theirs = [ring(me, (s + 1 - core) % 3)[0] for s in range(3)]
        self.send_sem = send_sem.at[index]
        self.recv_sems = [recv_sem.at[index, i] for i in range(RECEIVES)]
        self.sent = 0

    def take(self):
        return self.recv_sems.pop(0)

    def send(self, src, dst, device, recv_sem):
        self.sent += src.shape[0] * src.shape[1]
        pltpu.make_async_remote_copy(
            src_ref=src, dst_ref=dst, send_sem=self.send_sem, recv_sem=recv_sem,
            device_id=(device,), device_id_type=MESH,
        ).start()

    def wait(self, sem, rows, lanes):
        ref = self.part.at[0:rows, 0:lanes]
        pltpu.make_async_copy(ref, ref, sem).wait()

    def drain(self):
        tiles = self.sent // 1024
        self.wait(self.send_sem, tiles // 4 * 8, HID)
        if tiles % 4:
            self.wait(self.send_sem, 8, tiles % 4 * 128)

    def swap(self):
        self.swapped = {d: self.take() for d in ORDER}
        for d in ORDER:
            for s in range(3):
                q = self.sizes[s] // 4
                at = (self.theirs[s] + d) % 4 * q + self.first[s]
                self.send(
                    self.part.at[rows_at(self.other + at, q), :], self.work.at[rows_at(at, q), :], self.sibling,
                    self.swapped[d],
                )

    def scatter(self, blocks, sizes):
        k, send, work, plus, minus, one = 0, self.send, self.work, self.plus, self.minus, self.one
        up, down, rest = self.take(), self.take(), self.take()
        quarter = {}
        for d in ORDER:
            self.wait(self.swapped[d], sum(sizes), HID)
            for s in range(3):
                at, ahead = self.mine[s][k]
                q = sizes[s]
                local = blocks[s] + (at + d) % 4 * q
                rows = rows_at(local, q)
                quarter[s, d] = rows
                work[rows, :] = work[rows, :] + self.part[rows_at(self.base + local, q), :]
                here = pl.ds(0, q)
                if d == 2:
                    send(work.at[rows, LO], one.at[s, here, LO], ahead[1], up)
                    send(work.at[rows, HI], one.at[s, here, HI], ahead[3], down)
                elif d == 1:
                    send(work.at[rows, HI], plus.at[s, here, HI], ahead[1], rest)
                elif d == 3:
                    send(work.at[rows, LO], minus.at[s, here, LO], ahead[3], rest)
        yield
        for name, d, lanes, target, step in ((up, 1, LO, plus, 1), (down, 3, HI, minus, 3)):
            self.wait(name, sum(sizes), HID // 2)
            for s in range(3):
                rows, here = quarter[s, d], pl.ds(0, sizes[s])
                work[rows, lanes] = work[rows, lanes] + one[s, here, lanes]
                send(work.at[rows, lanes], target.at[s, here, lanes], self.mine[s][k][1][step], rest)
        yield
        self.wait(rest, 2 * sum(sizes), HID)
        for s in range(3):
            rows, here = quarter[s, 0], pl.ds(0, sizes[s])
            work[rows, :] = work[rows, :] + (plus[s, here, :] + minus[s, here, :])

    def scatter_straight(self, blocks, sizes):
        whole, work, sem = self.whole, self.work, self.take()
        for d in (2, 1, 3):
            for s in range(3):
                at, ahead = self.mine[s][1]
                rows = rows_at(blocks[s] + (at + d) % 4 * sizes[s], sizes[s])
                self.send(work.at[rows, ALL], whole.at[s, d - 1, pl.ds(0, sizes[s]), :], ahead[d], sem)
        yield
        self.wait(sem, 3 * sum(sizes), HID)
        for s in range(3):
            rows, here = rows_at(blocks[s] + self.mine[s][1][0] * sizes[s], sizes[s]), pl.ds(0, sizes[s])
            work[rows, :] = (work[rows, :] + whole[s, 1, here, :]) + (whole[s, 0, here, :] + whole[s, 2, here, :])

    def put(self, k, blocks, sizes, s, d, lanes, device, sem):
        start = self.base + blocks[s] + (self.mine[s][k][0] + d) % 4 * sizes[s]
        ref = self.tot.at[rows_at(start, sizes[s]), lanes]
        self.send(ref, ref, device, sem)

    def gather_straight(self, blocks, sizes):
        sem = self.take()
        for d in (2, 1, 3):
            for s in range(3):
                self.put(1, blocks, sizes, s, 0, ALL, self.mine[s][1][1][d], sem)
        yield
        self.wait(sem, 3 * sum(sizes), HID)

    def gather(self, blocks, sizes):
        up, down, rest, far, both = self.take(), self.take(), self.take(), self.take(), self.take()
        put = functools.partial(self.put, 0, blocks, sizes)

        def to_sibling(*quarters):
            for s in range(3):
                for d in quarters:
                    put(s, d, ALL, self.sibling, both)

        for lanes, step, sem in ((LO, 1, up), (HI, 3, down), (HI, 1, rest), (LO, 3, rest)):
            for s in range(3):
                put(s, 0, lanes, self.mine[s][0][1][step], sem)
        to_sibling(0)
        yield
        for sem, d, lanes, step in ((up, 3, LO, 1), (down, 1, HI, 3)):
            self.wait(sem, sum(sizes), HID // 2)
            for s in range(3):
                put(s, d, lanes, self.mine[s][0][1][step], far)
        yield
        self.wait(rest, sum(sizes), HID)
        to_sibling(3, 1)
        self.wait(far, sum(sizes), HID)
        to_sibling(2)
        yield
        self.wait(both, self.half, HID)

    def steps(self):
        size_a = [size // 4 for size in self.sizes]
        size_b = [size // 16 for size in self.sizes]
        block_a = self.first
        yield from self.scatter(block_a, size_a)
        block_b = [block_a[s] + self.mine[s][0][0] * size_a[s] for s in range(3)]
        yield from self.scatter_straight(block_b, size_b)
        block_c = [block_b[s] + self.mine[s][1][0] * size_b[s] for s in range(3)]

        piece, work, tot = self.piece, self.work, self.tot
        last, final = self.take(), self.take()
        for d in (2, 1, 3):
            for s in range(3):
                at, ahead = self.mine[s][2]
                self.send(
                    work.at[rows_at(block_c[s], size_b[s]), lanes_at((at + d) % 4)],
                    piece.at[s, d - 1, pl.ds(0, size_b[s]), :], ahead[d], last,
                )
        yield
        self.wait(last, 3 * sum(size_b), 128)
        for s in range(3):
            at, ahead = self.mine[s][2]
            here = pl.ds(0, size_b[s])
            got = work[rows_at(block_c[s], size_b[s]), lanes_at(at)] + (piece[s, 0, here, :] + piece[s, 2, here, :])
            rows = rows_at(self.base + block_c[s], size_b[s])
            tot[rows, lanes_at(at)] = got + piece[s, 1, here, :]
            for d in (2, 1, 3):
                ref = tot.at[rows, lanes_at(at)]
                self.send(ref, ref, ahead[d], final)
        yield
        self.wait(final, 3 * sum(size_b), 128)
        yield from self.gather_straight(block_b, size_b)
        yield from self.gather(block_a, size_a)
        yield


def wave_buffers(sizes):
    q, half = max(sizes) // 4, sum(sizes)
    return [
        pltpu.VMEM((half, HID), F32),
        pltpu.VMEM((3, q, HID), F32),
        pltpu.VMEM((3, q, HID), F32),
        pltpu.VMEM((3, q, HID), F32),
        pltpu.VMEM((3, 3, q // 4, HID), F32),
        pltpu.VMEM((3, 3, q // 4, 128), F32),
    ]


def in_hbm(x):
    return pltpu.with_memory_space_constraint(x, pltpu.HBM)


def main(*args):
    hbm = pl.BlockSpec(memory_space=pltpu.HBM)
    vm = pl.BlockSpec(memory_space=pltpu.VMEM)
    buffers = []
    for sizes, _ in WAVES:
        buffers += wave_buffers(sizes)
    return pl.pallas_call(
        main_kernel,
        name="gradients_and_sum",
        in_specs=[hbm] * 11,
        out_specs=[vm, vm],
        out_shape=[pltpu.VMEM((TOTAL_ROWS, HID), F32), pltpu.VMEM((1, ROWS), F32)],
        scratch_shapes=[
            pltpu.VMEM((FEAT, ROWS), BF16),
            pltpu.VMEM((FEAT, HID), BF16),
            pltpu.VMEM((1, HID), F32),
            pltpu.VMEM((HEADS, HID), BF16),
            pltpu.VMEM((1, HEADS), F32),
            pltpu.VMEM((1, ROWS), jnp.int32),
            pltpu.VMEM((ACT, ATOM, ROWS), F32),
            pltpu.VMEM((1, ROWS), jnp.int32),
            pltpu.VMEM((ATOM, ROWS), jnp.int32),
            pltpu.VMEM((ATOM, ROWS), F32),
            pltpu.VMEM((1, ROWS), F32),
            pltpu.VMEM((HEADS, HID), F32),
            pltpu.VMEM((HEAD, HID), BF16),
            pltpu.VMEM((1088, 128), F32),
            pltpu.VMEM((ATOM, 128), F32),
            pltpu.VMEM((ATOM, 128), F32),
            pltpu.VMEM((SLOT, ROWS), F32),
            pltpu.VMEM((ROWS, HID), BF16),
            pltpu.VMEM((HEAD, ROWS), BF16),
            pltpu.VMEM((ROWS, HID), BF16),
            pltpu.VMEM((1024, 128), F32),
            pltpu.VMEM((TOTAL_ROWS, HID), F32),
            pltpu.SemaphoreType.DMA((12,)),
            pltpu.SemaphoreType.DMA((len(WAVES),)),
            pltpu.SemaphoreType.DMA((len(WAVES), RECEIVES)),
            *buffers,
        ],
        compiler_params=pltpu.CompilerParams(
            vmem_limit_bytes=54 * 1024 * 1024, collective_id=0, has_side_effects=True
        ),
    )(*[in_hbm(x) for x in args])


def finish(tot, ce):
    hbm = pl.BlockSpec(memory_space=pltpu.HBM)
    vm = pl.BlockSpec(memory_space=pltpu.VMEM)
    return pl.pallas_call(
        finish_kernel,
        name="finish",
        in_specs=[vm, vm],
        out_specs=[hbm] * 6,
        out_shape=[
            jax.ShapeDtypeStruct((FEAT, HID), F32),
            jax.ShapeDtypeStruct((1, HID), F32),
            jax.ShapeDtypeStruct((HEADS, HID), F32),
            jax.ShapeDtypeStruct((1, HEADS), F32),
            jax.ShapeDtypeStruct((1, 1), F32),
            jax.ShapeDtypeStruct((1, ROWS), F32),
        ],
        scratch_shapes=[
            pltpu.VMEM((HEADS, HID), F32),
            pltpu.VMEM((1, HID), F32),
            pltpu.VMEM((1, HEADS), F32),
            pltpu.VMEM((1, 1), F32),
            pltpu.VMEM((1, ROWS), F32),
            pltpu.SemaphoreType.DMA((9,)),
        ],
        compiler_params=pltpu.CompilerParams(vmem_limit_bytes=8 * 1024 * 1024),
    )(tot, ce)


def on_device(features, w_one, b_one, w_two, b_two, action, target_probs, next_action, lower_idx, upper_frac, is_weight):
    tot, ce = main(
        features.T, w_one.T, b_one[None, :], w_two.T, b_two[None, :], action[None, :],
        target_probs.transpose(1, 2, 0), next_action[None, :], lower_idx.T, upper_frac.T, is_weight[None, :],
    )
    gw1, gb1, gw2, gb2, loss, prio = finish(tot, ce)
    return gw1.T, gb1[0], gw2.T, gb2[0], loss[0, 0], prio[0]


def solution(mesh):
    in_specs = (
        P("dp", None), P(), P(), P(), P(), P("dp"), P("dp", None, None), P("dp"), P("dp", None), P("dp", None), P("dp"),
    )
    out_specs = (P(), P(), P(), P(), P(), P("dp"))
    return jax.shard_map(on_device, mesh=mesh, in_specs=in_specs, out_specs=out_specs, check_vma=False)
```

```python
import functools

import jax
import jax.numpy as jnp
from jax import lax
from jax.experimental import pallas as pl
from jax.experimental.pallas import tpu as pltpu
from jax.sharding import PartitionSpec as P

MESH = pl.DeviceIdType.MESH
F32, BF16 = jnp.float32, jnp.bfloat16

FEAT, HID, ACT, ATOM, ROWS = 3136, 512, 18, 51, 1024
SLOT = 64
HEAD = ACT * SLOT
HEADS = ACT * ATOM

W1_AT = 928
B1_AT = W1_AT + FEAT
B2_AT = B1_AT + 1
TOP_AT = B2_AT + 2
LOSS_AT = TOP_AT + 1
TOTAL_ROWS = 4096
WAVES = (
    ((128, 128, 128), None),
    ((256, 128, 128), (2, 256)),
    ((256, 256, 256), (2, 384)),
    ((128, 128, 128), (2, 192)),
)
PLAN = "a0A1b0B12c0C1230123012301230132103203213230132"


def main_kernel(
    feat_hbm, w1_hbm, b1_hbm, w2_hbm, b2_hbm, act_hbm, tp_hbm, nact_hbm, low_hbm, frac_hbm, isw_hbm,
    tot, ce_ref,
    feat, w1, b1_ref, w2raw, b2_ref, act_ref, tp, nact_ref, low_ref, frac_ref, isw_ref,
    w2f, w2p, b2col, mlow, mhigh, proj, hid, glt, gp, gb2, part_ref, sems, send_sem, recv_sem, *buffers,
):
    me = lax.axis_index("dp")
    core = me % 2
    sibling = me + 1 - 2 * core
    left, right = slice(0, ROWS // 2), slice(ROWS // 2, ROWS)
    pairs = [(nact_hbm, nact_ref), (low_hbm, low_ref), (frac_hbm, frac_ref)]
    for t in range(4):
        cols = slice(256 * t, 256 * (t + 1))
        pairs.append((tp_hbm.at[:, :, cols], tp.at[:, :, cols]))
    pairs += [
        (w2_hbm, w2raw), (b2_hbm, b2_ref), (b1_hbm, b1_ref), (act_hbm, act_ref), (isw_hbm, isw_ref),
        (w1_hbm, w1), (feat_hbm.at[:, left], feat.at[:, left]), (feat_hbm.at[:, right], feat.at[:, right]),
    ]
    copies = [pltpu.make_async_copy(src, dst, sems.at[i]) for i, (src, dst) in enumerate(pairs)]
    for copy in copies[:7]:
        copy.start()
    near = [sibling]
    for axis in range(3):
        near += ring(me, axis)[1][1:]
    barrier = pltpu.get_barrier_semaphore()
    for device in near:
        pl.semaphore_signal(barrier, inc=1, device_id=(device,), device_id_type=MESH)

    for copy in copies[:4]:
        copy.wait()
    for copy in copies[7:]:
        copy.start()
    atom_row = lax.broadcasted_iota(jnp.int32, (56, 128), 0)
    proj[56:, :] = jnp.zeros((SLOT - 56, ROWS), F32)

    def project(t, carry):
        lanes = pl.ds(pl.multiple_of(t * 128, 128), 128)
        nact = nact_ref[:, lanes]
        probs = jnp.zeros((ATOM, 128), F32)
        for a in range(ACT):
            probs = jnp.where(nact == a, tp[a, :, lanes], probs)
        frac = frac_ref[:, lanes]
        mlow[...] = probs * (1.0 - frac)
        mhigh[...] = probs * frac
        low_sum = jnp.zeros((56, 128), F32)
        high_sum = jnp.zeros((56, 128), F32)
        for j in range(ATOM):
            hot = low_ref[pl.ds(j, 1), lanes] == atom_row
            low_sum = low_sum + jnp.where(hot, mlow[pl.ds(j, 1), :], 0.0)
            high_sum = high_sum + jnp.where(hot, mhigh[pl.ds(j, 1), :], 0.0)
        high_sum = jnp.where(atom_row == 0, 0.0, pltpu.roll(high_sum, 1, 0))
        proj[0:56, lanes] = low_sum + high_sum
        return carry

    lax.fori_loop(0, 2, project, 0)
    for t in range(1, 4):
        copies[3 + t].wait()
        lax.fori_loop(2 * t, 2 * t + 2, project, 0)

    copies[7].wait()
    copies[8].wait()
    w2f[...] = w2raw[...].astype(F32)
    wrow = lax.broadcasted_iota(jnp.int32, (SLOT, HID), 0)
    for a in range(ACT):
        if a < ACT - 1:
            block = w2f[ATOM * a : ATOM * a + SLOT, :]
        else:
            block = jnp.concatenate([w2f[ATOM * a : HEADS, :], jnp.zeros((SLOT - ATOM, HID), F32)], axis=0)
        w2p[SLOT * a : SLOT * (a + 1), :] = jnp.where(wrow < ATOM, block, 0.0).astype(BF16)
    b2row = jnp.concatenate([b2_ref[...], jnp.zeros((1, 1024 - HEADS), F32)], axis=1)
    b2col[0:1024, :] = jnp.broadcast_to(b2row, (128, 1024)).T
    b2col[1024:, :] = jnp.zeros((64, 128), F32)

    for copy in copies[9:13]:
        copy.wait()

    for t in range(2):
        copies[13 + t].wait()
        cols = slice(512 * t, 512 * (t + 1))
        pre = lax.dot_general(feat[:, cols], w1[...], (((0,), (0,)), ((), ())), preferred_element_type=F32)
        hid[cols, :] = jnp.maximum(pre + b1_ref[...], 0.0).astype(BF16)

    valid = lax.broadcasted_iota(jnp.int32, (SLOT, 256), 0) < ATOM

    def head(t, carry):
        loss, top = carry
        cols = slice(256 * t, 256 * (t + 1))
        logits = lax.dot_general(w2p[...], hid[cols, :], (((1,), (1,)), ((), ())), preferred_element_type=F32)
        action = act_ref[:, cols]
        chosen = jnp.zeros((SLOT, 256), F32)
        for a in range(ACT):
            bias = b2col[ATOM * a : ATOM * a + SLOT, :]
            biased = logits[SLOT * a : SLOT * (a + 1), :] + jnp.concatenate([bias, bias], axis=1)
            chosen = jnp.where(action == a, biased, chosen)
        chosen = jnp.where(valid, chosen, -1e30)
        shifted = chosen - jnp.max(chosen, axis=0, keepdims=True)
        expd = jnp.where(valid, jnp.exp(shifted), 0.0)
        log_probs = shifted - jnp.log(jnp.sum(expd, axis=0, keepdims=True))
        projected = proj[:, cols]
        cross = -jnp.sum(jnp.where(valid, projected * log_probs, 0.0), axis=0, keepdims=True)
        weight = isw_ref[:, cols]
        probs = jnp.where(valid, jnp.exp(log_probs), 0.0)
        grad = weight * (probs * jnp.sum(projected, axis=0, keepdims=True) - projected)
        grad16 = grad.astype(BF16)
        for a in range(ACT):
            glt[SLOT * a : SLOT * (a + 1), cols] = jnp.where(action == a, grad, 0.0).astype(BF16)
        ce_ref[:, cols] = cross
        return loss + weight * cross, jnp.maximum(top, cross)

    carry = (jnp.zeros((1, 256), F32), jnp.full((1, 256), -jnp.inf, F32))
    for t in range(ROWS // 256):
        carry = head(t, carry)
    loss_row, top_row = carry

    group = 6
    for g in range(ACT // group):
        rows = group * SLOT
        gl = glt[g * rows : (g + 1) * rows, :]
        gw2 = lax.dot_general(gl, hid[...], (((1,), (0,)), ((), ())), preferred_element_type=F32)
        for i in range(group):
            a = g * group + i
            part_ref[ATOM * a : ATOM * (a + 1), :] = gw2[SLOT * i : SLOT * i + ATOM, :]
    part_ref[HEADS:W1_AT, :] = jnp.zeros((W1_AT - HEADS, HID), F32)

    pl.semaphore_wait(barrier, len(near))
    waves, row, at = [], 0, 0
    for i, (sizes, _) in enumerate(WAVES):
        waves.append(Wave(i, sizes, row, me, core, send_sem, recv_sem, part_ref, tot, buffers[6 * i : 6 * (i + 1)]))
        row += 2 * sum(sizes)
    assert row == TOTAL_ROWS
    waves[0].swap()

    def back(t, gb1):
        cols = pl.ds(pl.multiple_of(t * 512, 512), 512)
        gh = lax.dot_general(glt[:, cols], w2p[...], (((0,), (0,)), ((), ())), preferred_element_type=F32)
        g16 = jnp.where(hid[cols, :].astype(F32) > 0.0, gh, 0.0).astype(BF16)
        gp[cols, :] = g16
        return gb1 + jnp.sum(g16.astype(F32), axis=0, keepdims=True)

    gb1 = lax.fori_loop(0, ROWS // 512, back, jnp.zeros((1, HID), F32))

    def grad_w1(wave, half, tiles, size):
        low = wave.row + half * wave.half
        start = jnp.maximum(low - W1_AT, 0)
        span = jnp.minimum(low + wave.half - W1_AT, FEAT) - start

        def tile(i, carry):
            at = start + jnp.minimum(i * size, span - size)
            rows = pl.ds(pl.multiple_of(at, 16), size)
            out = pl.ds(pl.multiple_of(at + W1_AT, 16), size)
            part_ref[out, :] = jnp.dot(feat[rows, :], gp[...], preferred_element_type=F32)
            return carry

        lax.fori_loop(0, tiles, tile, 0)

    def tail_rows():
        for a in range(ACT):
            ga = glt[SLOT * a : SLOT * (a + 1), :].astype(F32)
            gb2[ATOM * a : ATOM * (a + 1), :] = jnp.broadcast_to(jnp.sum(ga, axis=1, keepdims=True), (SLOT, 128))[:ATOM]
        gb2[HEADS:, :] = jnp.zeros((1024 - HEADS, 128), F32)
        gb2_row = gb2[...].T[0:1, :]
        lane = lax.broadcasted_iota(jnp.int32, (1, HID), 1)
        top = jnp.max(top_row)
        loss = jnp.sum(loss_row)
        part_ref[B1_AT:, :] = jnp.concatenate(
            [
                gb1,
                gb2_row[:, :HID],
                gb2_row[:, HID:],
                jnp.where(lane == me, top, 0.0),
                jnp.where(lane == 0, loss, 0.0),
                jnp.zeros((TOTAL_ROWS - LOSS_AT - 1, HID), F32),
            ],
            axis=0,
        )

    steps = [wave.steps() for wave in waves]

    for token in PLAN:
        i = "0ABCD".find(token.upper())
        if i > 0:
            other = token.islower()
            if other and i == len(waves) - 1:
                tail_rows()
            grad_w1(waves[i], 1 - core if other else core, *WAVES[i][1])
            if other:
                waves[i].swap()
        else:
            next(steps[int(token)])
    for wave in waves:
        wave.drain()


def finish_kernel(
    tot, ce, w1_out, b1_out, w2_out, b2_out, loss_out, prio_out, w2_copy, b1_copy, b2_copy, loss_copy, prio_copy, sems,
):
    copies = []

    def copy_out(src, dst):
        copies.append(pltpu.make_async_copy(src, dst, sems.at[len(copies)]))
        copies[-1].start()

    w2_copy[...] = tot[:HEADS, :]
    copy_out(w2_copy, w2_out)
    for i in range(4):
        copy_out(tot.at[pl.ds(W1_AT + 784 * i, 784), :], w1_out.at[pl.ds(784 * i, 784), :])
    b1_copy[...] = tot[B1_AT : B1_AT + 1, :]
    copy_out(b1_copy, b1_out)
    b2_copy[...] = jnp.concatenate([tot[B2_AT : B2_AT + 1, :], tot[B2_AT + 1 : B2_AT + 2, :]], axis=1)[:, :HEADS]
    copy_out(b2_copy, b2_out)
    loss_copy[...] = tot[LOSS_AT : LOSS_AT + 1, 0:1] * (1.0 / (ROWS * 128))
    copy_out(loss_copy, loss_out)
    top = jnp.max(tot[TOP_AT : TOP_AT + 1, 0:128])
    prio_copy[...] = ce[...] / jnp.maximum(top, 1.0)
    copy_out(prio_copy, prio_out)
    for copy in copies:
        copy.wait()


RECEIVES = 16
LO, HI, ALL = slice(0, HID // 2), slice(HID // 2, HID), slice(0, HID)
ORDER = (2, 1, 3, 0)


def rows_at(start, size):
    return pl.ds(pl.multiple_of(start, 8), size)


def lanes_at(p):
    return pl.ds(pl.multiple_of(p * 128, 128), 128)


def ring(me, axis):
    stride = 32 - 33 * axis + 9 * axis * axis
    at = (me // stride) % 4
    return at, [me + stride * ((at + d) % 4 - at) for d in range(4)]


class Wave:
    def __init__(self, index, sizes, row, me, core, send_sem, recv_sem, part, tot, buffers):
        self.row, self.half, self.part, self.tot = row, sum(sizes), part, tot
        self.work, self.plus, self.minus, self.one, self.whole, self.piece = buffers
        self.sizes = sizes
        self.first = [sum(sizes[:s]) for s in range(3)]
        self.base = row + core * self.half
        self.other = row + (1 - core) * self.half
        self.sibling = me + 1 - 2 * core
        self.mine = [[ring(me, (s + k + core) % 3) for k in range(3)] for s in range(3)]
        self.theirs = [ring(me, (s + 1 - core) % 3)[0] for s in range(3)]
        self.send_sem = send_sem.at[index]
        self.recv_sems = [recv_sem.at[index, i] for i in range(RECEIVES)]
        self.sent = 0

    def take(self):
        return self.recv_sems.pop(0)

    def send(self, src, dst, device, recv_sem):
        self.sent += src.shape[0] * src.shape[1]
        pltpu.make_async_remote_copy(
            src_ref=src, dst_ref=dst, send_sem=self.send_sem, recv_sem=recv_sem,
            device_id=(device,), device_id_type=MESH,
        ).start()

    def wait(self, sem, rows, lanes):
        ref = self.part.at[0:rows, 0:lanes]
        pltpu.make_async_copy(ref, ref, sem).wait()

    def drain(self):
        tiles = self.sent // 1024
        self.wait(self.send_sem, tiles // 4 * 8, HID)
        if tiles % 4:
            self.wait(self.send_sem, 8, tiles % 4 * 128)

    def swap(self):
        self.swapped = {d: self.take() for d in ORDER}
        for d in ORDER:
            for s in range(3):
                q = self.sizes[s] // 4
                at = (self.theirs[s] + d) % 4 * q + self.first[s]
                self.send(
                    self.part.at[rows_at(self.other + at, q), :], self.work.at[rows_at(at, q), :], self.sibling,
                    self.swapped[d],
                )

    def scatter(self, blocks, sizes):
        k, send, work, plus, minus, one = 0, self.send, self.work, self.plus, self.minus, self.one
        up, down, rest = self.take(), self.take(), self.take()
        quarter = {}
        for d in ORDER:
            self.wait(self.swapped[d], sum(sizes), HID)
            for s in range(3):
                at, ahead = self.mine[s][k]
                q = sizes[s]
                local = blocks[s] + (at + d) % 4 * q
                rows = rows_at(local, q)
                quarter[s, d] = rows
                work[rows, :] = work[rows, :] + self.part[rows_at(self.base + local, q), :]
                here = pl.ds(0, q)
                if d == 2:
                    send(work.at[rows, LO], one.at[s, here, LO], ahead[1], up)
                    send(work.at[rows, HI], one.at[s, here, HI], ahead[3], down)
                elif d == 1:
                    send(work.at[rows, HI], plus.at[s, here, HI], ahead[1], rest)
                elif d == 3:
                    send(work.at[rows, LO], minus.at[s, here, LO], ahead[3], rest)
        yield
        for name, d, lanes, target, step in ((up, 1, LO, plus, 1), (down, 3, HI, minus, 3)):
            self.wait(name, sum(sizes), HID // 2)
            for s in range(3):
                rows, here = quarter[s, d], pl.ds(0, sizes[s])
                work[rows, lanes] = work[rows, lanes] + one[s, here, lanes]
                send(work.at[rows, lanes], target.at[s, here, lanes], self.mine[s][k][1][step], rest)
        yield
        self.wait(rest, 2 * sum(sizes), HID)
        for s in range(3):
            rows, here = quarter[s, 0], pl.ds(0, sizes[s])
            work[rows, :] = work[rows, :] + (plus[s, here, :] + minus[s, here, :])

    def scatter_straight(self, blocks, sizes):
        whole, work, sem = self.whole, self.work, self.take()
        for d in (2, 1, 3):
            for s in range(3):
                at, ahead = self.mine[s][1]
                rows = rows_at(blocks[s] + (at + d) % 4 * sizes[s], sizes[s])
                self.send(work.at[rows, ALL], whole.at[s, d - 1, pl.ds(0, sizes[s]), :], ahead[d], sem)
        yield
        self.wait(sem, 3 * sum(sizes), HID)
        for s in range(3):
            rows, here = rows_at(blocks[s] + self.mine[s][1][0] * sizes[s], sizes[s]), pl.ds(0, sizes[s])
            work[rows, :] = (work[rows, :] + whole[s, 1, here, :]) + (whole[s, 0, here, :] + whole[s, 2, here, :])

    def put(self, k, blocks, sizes, s, d, lanes, device, sem):
        start = self.base + blocks[s] + (self.mine[s][k][0] + d) % 4 * sizes[s]
        ref = self.tot.at[rows_at(start, sizes[s]), lanes]
        self.send(ref, ref, device, sem)

    def gather_straight(self, blocks, sizes):
        sem = self.take()
        for d in (2, 1, 3):
            for s in range(3):
                self.put(1, blocks, sizes, s, 0, ALL, self.mine[s][1][1][d], sem)
        yield
        self.wait(sem, 3 * sum(sizes), HID)

    def gather(self, blocks, sizes):
        up, down, rest, far, both = self.take(), self.take(), self.take(), self.take(), self.take()
        put = functools.partial(self.put, 0, blocks, sizes)

        def to_sibling(*quarters):
            for s in range(3):
                for d in quarters:
                    put(s, d, ALL, self.sibling, both)

        for lanes, step, sem in ((LO, 1, up), (HI, 3, down), (HI, 1, rest), (LO, 3, rest)):
            for s in range(3):
                put(s, 0, lanes, self.mine[s][0][1][step], sem)
        to_sibling(0)
        yield
        for sem, d, lanes, step in ((up, 3, LO, 1), (down, 1, HI, 3)):
            self.wait(sem, sum(sizes), HID // 2)
            for s in range(3):
                put(s, d, lanes, self.mine[s][0][1][step], far)
        yield
        self.wait(rest, sum(sizes), HID)
        to_sibling(3, 1)
        self.wait(far, sum(sizes), HID)
        to_sibling(2)
        yield
        self.wait(both, self.half, HID)

    def steps(self):
        size_a = [size // 4 for size in self.sizes]
        size_b = [size // 16 for size in self.sizes]
        block_a = self.first
        yield from self.scatter(block_a, size_a)
        block_b = [block_a[s] + self.mine[s][0][0] * size_a[s] for s in range(3)]
        yield from self.scatter_straight(block_b, size_b)
        block_c = [block_b[s] + self.mine[s][1][0] * size_b[s] for s in range(3)]

        piece, work, tot = self.piece, self.work, self.tot
        last, final = self.take(), self.take()
        for d in (2, 1, 3):
            for s in range(3):
                at, ahead = self.mine[s][2]
                self.send(
                    work.at[rows_at(block_c[s], size_b[s]), lanes_at((at + d) % 4)],
                    piece.at[s, d - 1, pl.ds(0, size_b[s]), :], ahead[d], last,
                )
        yield
        self.wait(last, 3 * sum(size_b), 128)
        for s in range(3):
            at, ahead = self.mine[s][2]
            here = pl.ds(0, size_b[s])
            got = work[rows_at(block_c[s], size_b[s]), lanes_at(at)] + (piece[s, 0, here, :] + piece[s, 2, here, :])
            rows = rows_at(self.base + block_c[s], size_b[s])
            tot[rows, lanes_at(at)] = got + piece[s, 1, here, :]
            for d in (2, 1, 3):
                ref = tot.at[rows, lanes_at(at)]
                self.send(ref, ref, ahead[d], final)
        yield
        self.wait(final, 3 * sum(size_b), 128)
        yield from self.gather_straight(block_b, size_b)
        yield from self.gather(block_a, size_a)
        yield


def wave_buffers(sizes):
    q, half = max(sizes) // 4, sum(sizes)
    return [
        pltpu.VMEM((half, HID), F32),
        pltpu.VMEM((3, q, HID), F32),
        pltpu.VMEM((3, q, HID), F32),
        pltpu.VMEM((3, q, HID), F32),
        pltpu.VMEM((3, 3, q // 4, HID), F32),
        pltpu.VMEM((3, 3, q // 4, 128), F32),
    ]


def in_hbm(x):
    return pltpu.with_memory_space_constraint(x, pltpu.HBM)


def main(*args):
    hbm = pl.BlockSpec(memory_space=pltpu.HBM)
    vm = pl.BlockSpec(memory_space=pltpu.VMEM)
    buffers = []
    for sizes, _ in WAVES:
        buffers += wave_buffers(sizes)
    return pl.pallas_call(
        main_kernel,
        name="gradients_and_sum",
        in_specs=[hbm] * 11,
        out_specs=[vm, vm],
        out_shape=[pltpu.VMEM((TOTAL_ROWS, HID), F32), pltpu.VMEM((1, ROWS), F32)],
        scratch_shapes=[
            pltpu.VMEM((FEAT, ROWS), BF16),
            pltpu.VMEM((FEAT, HID), BF16),
            pltpu.VMEM((1, HID), F32),
            pltpu.VMEM((HEADS, HID), BF16),
            pltpu.VMEM((1, HEADS), F32),
            pltpu.VMEM((1, ROWS), jnp.int32),
            pltpu.VMEM((ACT, ATOM, ROWS), F32),
            pltpu.VMEM((1, ROWS), jnp.int32),
            pltpu.VMEM((ATOM, ROWS), jnp.int32),
            pltpu.VMEM((ATOM, ROWS), F32),
            pltpu.VMEM((1, ROWS), F32),
            pltpu.VMEM((HEADS, HID), F32),
            pltpu.VMEM((HEAD, HID), BF16),
            pltpu.VMEM((1088, 128), F32),
            pltpu.VMEM((ATOM, 128), F32),
            pltpu.VMEM((ATOM, 128), F32),
            pltpu.VMEM((SLOT, ROWS), F32),
            pltpu.VMEM((ROWS, HID), BF16),
            pltpu.VMEM((HEAD, ROWS), BF16),
            pltpu.VMEM((ROWS, HID), BF16),
            pltpu.VMEM((1024, 128), F32),
            pltpu.VMEM((TOTAL_ROWS, HID), F32),
            pltpu.SemaphoreType.DMA((15,)),
            pltpu.SemaphoreType.DMA((len(WAVES),)),
            pltpu.SemaphoreType.DMA((len(WAVES), RECEIVES)),
            *buffers,
        ],
        compiler_params=pltpu.CompilerParams(
            vmem_limit_bytes=54 * 1024 * 1024, collective_id=0, has_side_effects=True
        ),
    )(*[in_hbm(x) for x in args])


def finish(tot, ce):
    hbm = pl.BlockSpec(memory_space=pltpu.HBM)
    vm = pl.BlockSpec(memory_space=pltpu.VMEM)
    return pl.pallas_call(
        finish_kernel,
        name="finish",
        in_specs=[vm, vm],
        out_specs=[hbm] * 6,
        out_shape=[
            jax.ShapeDtypeStruct((FEAT, HID), F32),
            jax.ShapeDtypeStruct((1, HID), F32),
            jax.ShapeDtypeStruct((HEADS, HID), F32),
            jax.ShapeDtypeStruct((1, HEADS), F32),
            jax.ShapeDtypeStruct((1, 1), F32),
            jax.ShapeDtypeStruct((1, ROWS), F32),
        ],
        scratch_shapes=[
            pltpu.VMEM((HEADS, HID), F32),
            pltpu.VMEM((1, HID), F32),
            pltpu.VMEM((1, HEADS), F32),
            pltpu.VMEM((1, 1), F32),
            pltpu.VMEM((1, ROWS), F32),
            pltpu.SemaphoreType.DMA((9,)),
        ],
        compiler_params=pltpu.CompilerParams(vmem_limit_bytes=8 * 1024 * 1024),
    )(tot, ce)


def on_device(features, w_one, b_one, w_two, b_two, action, target_probs, next_action, lower_idx, upper_frac, is_weight):
    tot, ce = main(
        features.T, w_one.T, b_one[None, :], w_two.T, b_two[None, :], action[None, :],
        target_probs.transpose(1, 2, 0), next_action[None, :], lower_idx.T, upper_frac.T, is_weight[None, :],
    )
    gw1, gb1, gw2, gb2, loss, prio = finish(tot, ce)
    return gw1.T, gb1[0], gw2.T, gb2[0], loss[0, 0], prio[0]


def solution(mesh):
    in_specs = (
        P("dp", None), P(), P(), P(), P(), P("dp"), P("dp", None, None), P("dp"), P("dp", None), P("dp", None), P("dp"),
    )
    out_specs = (P(), P(), P(), P(), P(), P("dp"))
    return jax.shard_map(on_device, mesh=mesh, in_specs=in_specs, out_specs=out_specs, check_vma=False)
```

```python
import functools

import jax
import jax.numpy as jnp
from jax import lax
from jax.experimental import pallas as pl
from jax.experimental.pallas import tpu as pltpu
from jax.sharding import PartitionSpec as P

MESH = pl.DeviceIdType.MESH
F32, BF16 = jnp.float32, jnp.bfloat16

FEAT, HID, ACT, ATOM, ROWS = 3136, 512, 18, 51, 1024
SLOT = 64
HEAD = ACT * SLOT
HEADS = ACT * ATOM

W1_AT = 928
B1_AT = W1_AT + FEAT
B2_AT = B1_AT + 1
TOP_AT = B2_AT + 2
LOSS_AT = TOP_AT + 1
TOTAL_ROWS = 4096
WAVES = (
    ((128, 128, 128), None),
    ((256, 128, 128), (2, 256)),
    ((256, 256, 256), (2, 384)),
    ((128, 128, 128), (2, 192)),
)
PLAN = "a0A1b0B12c0C1230123012301230132103203213230132"


def main_kernel(
    feat_hbm, w1_hbm, b1_hbm, w2_hbm, b2_hbm, act_hbm, tp_hbm, nact_hbm, low_hbm, frac_hbm, isw_hbm,
    tot, ce_ref,
    feat, w1, b1_ref, w2raw, b2_ref, act_ref, tp, nact_ref, low_ref, frac_ref, isw_ref,
    w2f, w2p, b2col, mlow, mhigh, proj, hid, glt, gp, gb2, part_ref, sems, send_sem, recv_sem, *buffers,
):
    me = lax.axis_index("dp")
    core = me % 2
    sibling = me + 1 - 2 * core
    left, right = slice(0, ROWS // 2), slice(ROWS // 2, ROWS)
    pairs = [(nact_hbm, nact_ref), (low_hbm, low_ref), (frac_hbm, frac_ref)]
    for t in range(4):
        cols = slice(256 * t, 256 * (t + 1))
        pairs.append((tp_hbm.at[:, :, cols], tp.at[:, :, cols]))
    pairs += [
        (w2_hbm, w2raw), (b2_hbm, b2_ref), (b1_hbm, b1_ref), (act_hbm, act_ref), (isw_hbm, isw_ref),
        (w1_hbm, w1), (feat_hbm.at[:, left], feat.at[:, left]), (feat_hbm.at[:, right], feat.at[:, right]),
    ]
    copies = [pltpu.make_async_copy(src, dst, sems.at[i]) for i, (src, dst) in enumerate(pairs)]
    for copy in copies[:7]:
        copy.start()
    near = [sibling]
    for axis in range(3):
        near += ring(me, axis)[1][1:]
    barrier = pltpu.get_barrier_semaphore()
    for device in near:
        pl.semaphore_signal(barrier, inc=1, device_id=(device,), device_id_type=MESH)

    for copy in copies[:4]:
        copy.wait()
    for copy in copies[7:]:
        copy.start()
    atom_row = lax.broadcasted_iota(jnp.int32, (56, 128), 0)
    proj[56:, :] = jnp.zeros((SLOT - 56, ROWS), F32)

    def project(t, carry):
        lanes = pl.ds(pl.multiple_of(t * 128, 128), 128)
        nact = nact_ref[:, lanes]
        probs = jnp.zeros((ATOM, 128), F32)
        for a in range(ACT):
            probs = jnp.where(nact == a, tp[a, :, lanes], probs)
        frac = frac_ref[:, lanes]
        mlow[...] = probs * (1.0 - frac)
        mhigh[...] = probs * frac
        low_sum = jnp.zeros((56, 128), F32)
        high_sum = jnp.zeros((56, 128), F32)
        for j in range(ATOM):
            hot = low_ref[pl.ds(j, 1), lanes] == atom_row
            low_sum = low_sum + jnp.where(hot, mlow[pl.ds(j, 1), :], 0.0)
            high_sum = high_sum + jnp.where(hot, mhigh[pl.ds(j, 1), :], 0.0)
        high_sum = jnp.where(atom_row == 0, 0.0, pltpu.roll(high_sum, 1, 0))
        proj[0:56, lanes] = low_sum + high_sum
        return carry

    lax.fori_loop(0, 2, project, 0)
    for t in range(1, 4):
        copies[3 + t].wait()
        lax.fori_loop(2 * t, 2 * t + 2, project, 0)

    copies[7].wait()
    copies[8].wait()
    w2f[...] = w2raw[...].astype(F32)
    wrow = lax.broadcasted_iota(jnp.int32, (SLOT, HID), 0)
    for a in range(ACT):
        if a < ACT - 1:
            block = w2f[ATOM * a : ATOM * a + SLOT, :]
        else:
            block = jnp.concatenate([w2f[ATOM * a : HEADS, :], jnp.zeros((SLOT - ATOM, HID), F32)], axis=0)
        w2p[SLOT * a : SLOT * (a + 1), :] = jnp.where(wrow < ATOM, block, 0.0).astype(BF16)
    b2row = jnp.concatenate([b2_ref[...], jnp.zeros((1, 1024 - HEADS), F32)], axis=1)
    b2col[0:1024, :] = jnp.broadcast_to(b2row, (128, 1024)).T
    b2col[1024:, :] = jnp.zeros((64, 128), F32)

    for copy in copies[9:13]:
        copy.wait()

    for t in range(2):
        copies[13 + t].wait()
        cols = slice(512 * t, 512 * (t + 1))
        pre = lax.dot_general(feat[:, cols], w1[...], (((0,), (0,)), ((), ())), preferred_element_type=F32)
        hid[cols, :] = jnp.maximum(pre + b1_ref[...], 0.0).astype(BF16)

    valid = lax.broadcasted_iota(jnp.int32, (SLOT, 256), 0) < ATOM

    def head(t, carry):
        loss, top = carry
        cols = slice(256 * t, 256 * (t + 1))
        logits = lax.dot_general(w2p[...], hid[cols, :], (((1,), (1,)), ((), ())), preferred_element_type=F32)
        action = act_ref[:, cols]
        chosen = jnp.zeros((SLOT, 256), F32)
        for a in range(ACT):
            bias = b2col[ATOM * a : ATOM * a + SLOT, :]
            biased = logits[SLOT * a : SLOT * (a + 1), :] + jnp.concatenate([bias, bias], axis=1)
            chosen = jnp.where(action == a, biased, chosen)
        chosen = jnp.where(valid, chosen, -1e30)
        shifted = chosen - jnp.max(chosen, axis=0, keepdims=True)
        expd = jnp.where(valid, jnp.exp(shifted), 0.0)
        log_probs = shifted - jnp.log(jnp.sum(expd, axis=0, keepdims=True))
        projected = proj[:, cols]
        cross = -jnp.sum(jnp.where(valid, projected * log_probs, 0.0), axis=0, keepdims=True)
        weight = isw_ref[:, cols]
        probs = jnp.where(valid, jnp.exp(log_probs), 0.0)
        grad = weight * (probs * jnp.sum(projected, axis=0, keepdims=True) - projected)
        grad16 = grad.astype(BF16)
        for a in range(ACT):
            glt[SLOT * a : SLOT * (a + 1), cols] = jnp.where(action == a, grad, 0.0).astype(BF16)
        ce_ref[:, cols] = cross
        return loss + weight * cross, jnp.maximum(top, cross)

    carry = (jnp.zeros((1, 256), F32), jnp.full((1, 256), -jnp.inf, F32))
    for t in range(ROWS // 256):
        carry = head(t, carry)
    loss_row, top_row = carry

    group = 6
    for g in range(ACT // group):
        rows = group * SLOT
        gl = glt[g * rows : (g + 1) * rows, :]
        gw2 = lax.dot_general(gl, hid[...], (((1,), (0,)), ((), ())), preferred_element_type=F32)
        for i in range(group):
            a = g * group + i
            part_ref[ATOM * a : ATOM * (a + 1), :] = gw2[SLOT * i : SLOT * i + ATOM, :]
    part_ref[HEADS:W1_AT, :] = jnp.zeros((W1_AT - HEADS, HID), F32)

    pl.semaphore_wait(barrier, len(near))
    waves, row, at = [], 0, 0
    for i, (sizes, _) in enumerate(WAVES):
        waves.append(Wave(i, sizes, row, me, core, send_sem, recv_sem, part_ref, tot, buffers[6 * i : 6 * (i + 1)]))
        row += 2 * sum(sizes)
    assert row == TOTAL_ROWS
    waves[0].swap()

    def back(t, gb1):
        cols = pl.ds(pl.multiple_of(t * 512, 512), 512)
        gh = lax.dot_general(glt[:, cols], w2p[...], (((0,), (0,)), ((), ())), preferred_element_type=F32)
        g16 = jnp.where(hid[cols, :].astype(F32) > 0.0, gh, 0.0).astype(BF16)
        gp[cols, :] = g16
        return gb1 + jnp.sum(g16.astype(F32), axis=0, keepdims=True)

    gb1 = lax.fori_loop(0, ROWS // 512, back, jnp.zeros((1, HID), F32))

    def grad_w1(wave, half, tiles, size):
        low = wave.row + half * wave.half
        start = jnp.maximum(low - W1_AT, 0)
        span = jnp.minimum(low + wave.half - W1_AT, FEAT) - start

        def tile(i, carry):
            at = start + jnp.minimum(i * size, span - size)
            rows = pl.ds(pl.multiple_of(at, 16), size)
            out = pl.ds(pl.multiple_of(at + W1_AT, 16), size)
            part_ref[out, :] = jnp.dot(feat[rows, :], gp[...], preferred_element_type=F32)
            return carry

        lax.fori_loop(0, tiles, tile, 0)

    def tail_rows():
        for a in range(ACT):
            ga = glt[SLOT * a : SLOT * (a + 1), :].astype(F32)
            gb2[ATOM * a : ATOM * (a + 1), :] = jnp.broadcast_to(jnp.sum(ga, axis=1, keepdims=True), (SLOT, 128))[:ATOM]
        gb2[HEADS:, :] = jnp.zeros((1024 - HEADS, 128), F32)
        gb2_row = gb2[...].T[0:1, :]
        lane = lax.broadcasted_iota(jnp.int32, (1, HID), 1)
        top = jnp.max(top_row)
        loss = jnp.sum(loss_row)
        part_ref[B1_AT:, :] = jnp.concatenate(
            [
                gb1,
                gb2_row[:, :HID],
                gb2_row[:, HID:],
                jnp.where(lane == me, top, 0.0),
                jnp.where(lane == 0, loss, 0.0),
                jnp.zeros((TOTAL_ROWS - LOSS_AT - 1, HID), F32),
            ],
            axis=0,
        )

    steps = [wave.steps() for wave in waves]

    for token in PLAN:
        i = "0ABCD".find(token.upper())
        if i > 0:
            other = token.islower()
            if other and i == len(waves) - 1:
                tail_rows()
            grad_w1(waves[i], 1 - core if other else core, *WAVES[i][1])
            if other:
                waves[i].swap()
        else:
            next(steps[int(token)])
    for wave in waves:
        wave.drain()


def finish_kernel(
    tot, ce, w1_out, b1_out, w2_out, b2_out, loss_out, prio_out, w2_copy, b1_copy, b2_copy, loss_copy, prio_copy, sems,
):
    copies = []

    def copy_out(src, dst):
        copies.append(pltpu.make_async_copy(src, dst, sems.at[len(copies)]))
        copies[-1].start()

    for i in range(4):
        copy_out(tot.at[pl.ds(W1_AT + 784 * i, 784), :], w1_out.at[pl.ds(784 * i, 784), :])
    w2_copy[...] = tot[:HEADS, :]
    copy_out(w2_copy, w2_out)
    b1_copy[...] = tot[B1_AT : B1_AT + 1, :]
    copy_out(b1_copy, b1_out)
    b2_copy[...] = jnp.concatenate([tot[B2_AT : B2_AT + 1, :], tot[B2_AT + 1 : B2_AT + 2, :]], axis=1)[:, :HEADS]
    copy_out(b2_copy, b2_out)
    loss_copy[...] = tot[LOSS_AT : LOSS_AT + 1, 0:1] * (1.0 / (ROWS * 128))
    copy_out(loss_copy, loss_out)
    top = jnp.max(tot[TOP_AT : TOP_AT + 1, 0:128])
    prio_copy[...] = ce[...] / jnp.maximum(top, 1.0)
    copy_out(prio_copy, prio_out)
    for copy in copies:
        copy.wait()


RECEIVES = 16
LO, HI, ALL = slice(0, HID // 2), slice(HID // 2, HID), slice(0, HID)
ORDER = (2, 1, 3, 0)


def rows_at(start, size):
    return pl.ds(pl.multiple_of(start, 8), size)


def lanes_at(p):
    return pl.ds(pl.multiple_of(p * 128, 128), 128)


def ring(me, axis):
    stride = 32 - 33 * axis + 9 * axis * axis
    at = (me // stride) % 4
    return at, [me + stride * ((at + d) % 4 - at) for d in range(4)]


class Wave:
    def __init__(self, index, sizes, row, me, core, send_sem, recv_sem, part, tot, buffers):
        self.row, self.half, self.part, self.tot = row, sum(sizes), part, tot
        self.work, self.plus, self.minus, self.one, self.whole, self.piece = buffers
        self.sizes = sizes
        self.first = [sum(sizes[:s]) for s in range(3)]
        self.base = row + core * self.half
        self.other = row + (1 - core) * self.half
        self.sibling = me + 1 - 2 * core
        self.mine = [[ring(me, (s + k + core) % 3) for k in range(3)] for s in range(3)]
        self.theirs = [ring(me, (s + 1 - core) % 3)[0] for s in range(3)]
        self.send_sem = send_sem.at[index]
        self.recv_sems = [recv_sem.at[index, i] for i in range(RECEIVES)]
        self.sent = 0

    def take(self):
        return self.recv_sems.pop(0)

    def send(self, src, dst, device, recv_sem):
        self.sent += src.shape[0] * src.shape[1]
        pltpu.make_async_remote_copy(
            src_ref=src, dst_ref=dst, send_sem=self.send_sem, recv_sem=recv_sem,
            device_id=(device,), device_id_type=MESH,
        ).start()

    def wait(self, sem, rows, lanes):
        ref = self.part.at[0:rows, 0:lanes]
        pltpu.make_async_copy(ref, ref, sem).wait()

    def drain(self):
        tiles = self.sent // 1024
        self.wait(self.send_sem, tiles // 4 * 8, HID)
        if tiles % 4:
            self.wait(self.send_sem, 8, tiles % 4 * 128)

    def swap(self):
        self.swapped = {d: self.take() for d in ORDER}
        for d in ORDER:
            for s in range(3):
                q = self.sizes[s] // 4
                at = (self.theirs[s] + d) % 4 * q + self.first[s]
                self.send(
                    self.part.at[rows_at(self.other + at, q), :], self.work.at[rows_at(at, q), :], self.sibling,
                    self.swapped[d],
                )

    def scatter(self, blocks, sizes):
        k, send, work, plus, minus, one = 0, self.send, self.work, self.plus, self.minus, self.one
        up, down, rest = self.take(), self.take(), self.take()
        quarter = {}
        for d in ORDER:
            self.wait(self.swapped[d], sum(sizes), HID)
            for s in range(3):
                at, ahead = self.mine[s][k]
                q = sizes[s]
                local = blocks[s] + (at + d) % 4 * q
                rows = rows_at(local, q)
                quarter[s, d] = rows
                work[rows, :] = work[rows, :] + self.part[rows_at(self.base + local, q), :]
                here = pl.ds(0, q)
                if d == 2:
                    send(work.at[rows, LO], one.at[s, here, LO], ahead[1], up)
                    send(work.at[rows, HI], one.at[s, here, HI], ahead[3], down)
                elif d == 1:
                    send(work.at[rows, HI], plus.at[s, here, HI], ahead[1], rest)
                elif d == 3:
                    send(work.at[rows, LO], minus.at[s, here, LO], ahead[3], rest)
        yield
        for name, d, lanes, target, step in ((up, 1, LO, plus, 1), (down, 3, HI, minus, 3)):
            self.wait(name, sum(sizes), HID // 2)
            for s in range(3):
                rows, here = quarter[s, d], pl.ds(0, sizes[s])
                work[rows, lanes] = work[rows, lanes] + one[s, here, lanes]
                send(work.at[rows, lanes], target.at[s, here, lanes], self.mine[s][k][1][step], rest)
        yield
        self.wait(rest, 2 * sum(sizes), HID)
        for s in range(3):
            rows, here = quarter[s, 0], pl.ds(0, sizes[s])
            work[rows, :] = work[rows, :] + (plus[s, here, :] + minus[s, here, :])

    def scatter_straight(self, blocks, sizes):
        whole, work, sem = self.whole, self.work, self.take()
        for d in (2, 1, 3):
            for s in range(3):
                at, ahead = self.mine[s][1]
                rows = rows_at(blocks[s] + (at + d) % 4 * sizes[s], sizes[s])
                self.send(work.at[rows, ALL], whole.at[s, d - 1, pl.ds(0, sizes[s]), :], ahead[d], sem)
        yield
        self.wait(sem, 3 * sum(sizes), HID)
        for s in range(3):
            rows, here = rows_at(blocks[s] + self.mine[s][1][0] * sizes[s], sizes[s]), pl.ds(0, sizes[s])
            work[rows, :] = (work[rows, :] + whole[s, 1, here, :]) + (whole[s, 0, here, :] + whole[s, 2, here, :])

    def put(self, k, blocks, sizes, s, d, lanes, device, sem):
        start = self.base + blocks[s] + (self.mine[s][k][0] + d) % 4 * sizes[s]
        ref = self.tot.at[rows_at(start, sizes[s]), lanes]
        self.send(ref, ref, device, sem)

    def gather_straight(self, blocks, sizes):
        sem = self.take()
        for d in (2, 1, 3):
            for s in range(3):
                self.put(1, blocks, sizes, s, 0, ALL, self.mine[s][1][1][d], sem)
        yield
        self.wait(sem, 3 * sum(sizes), HID)

    def gather(self, blocks, sizes):
        up, down, rest, far, both = self.take(), self.take(), self.take(), self.take(), self.take()
        put = functools.partial(self.put, 0, blocks, sizes)

        def to_sibling(*quarters):
            for s in range(3):
                for d in quarters:
                    put(s, d, ALL, self.sibling, both)

        for lanes, step, sem in ((LO, 1, up), (HI, 3, down), (HI, 1, rest), (LO, 3, rest)):
            for s in range(3):
                put(s, 0, lanes, self.mine[s][0][1][step], sem)
        to_sibling(0)
        yield
        for sem, d, lanes, step in ((up, 3, LO, 1), (down, 1, HI, 3)):
            self.wait(sem, sum(sizes), HID // 2)
            for s in range(3):
                put(s, d, lanes, self.mine[s][0][1][step], far)
        yield
        self.wait(rest, sum(sizes), HID)
        to_sibling(3, 1)
        self.wait(far, sum(sizes), HID)
        to_sibling(2)
        yield
        self.wait(both, self.half, HID)

    def steps(self):
        size_a = [size // 4 for size in self.sizes]
        size_b = [size // 16 for size in self.sizes]
        block_a = self.first
        yield from self.scatter(block_a, size_a)
        block_b = [block_a[s] + self.mine[s][0][0] * size_a[s] for s in range(3)]
        yield from self.scatter_straight(block_b, size_b)
        block_c = [block_b[s] + self.mine[s][1][0] * size_b[s] for s in range(3)]

        piece, work, tot = self.piece, self.work, self.tot
        last, final = self.take(), self.take()
        for d in (2, 1, 3):
            for s in range(3):
                at, ahead = self.mine[s][2]
                self.send(
                    work.at[rows_at(block_c[s], size_b[s]), lanes_at((at + d) % 4)],
                    piece.at[s, d - 1, pl.ds(0, size_b[s]), :], ahead[d], last,
                )
        yield
        self.wait(last, 3 * sum(size_b), 128)
        for s in range(3):
            at, ahead = self.mine[s][2]
            here = pl.ds(0, size_b[s])
            got = work[rows_at(block_c[s], size_b[s]), lanes_at(at)] + (piece[s, 0, here, :] + piece[s, 2, here, :])
            rows = rows_at(self.base + block_c[s], size_b[s])
            tot[rows, lanes_at(at)] = got + piece[s, 1, here, :]
            for d in (2, 1, 3):
                ref = tot.at[rows, lanes_at(at)]
                self.send(ref, ref, ahead[d], final)
        yield
        self.wait(final, 3 * sum(size_b), 128)
        yield from self.gather_straight(block_b, size_b)
        yield from self.gather(block_a, size_a)
        yield


def wave_buffers(sizes):
    q, half = max(sizes) // 4, sum(sizes)
    return [
        pltpu.VMEM((half, HID), F32),
        pltpu.VMEM((3, q, HID), F32),
        pltpu.VMEM((3, q, HID), F32),
        pltpu.VMEM((3, q, HID), F32),
        pltpu.VMEM((3, 3, q // 4, HID), F32),
        pltpu.VMEM((3, 3, q // 4, 128), F32),
    ]


def in_hbm(x):
    return pltpu.with_memory_space_constraint(x, pltpu.HBM)


def main(*args):
    hbm = pl.BlockSpec(memory_space=pltpu.HBM)
    vm = pl.BlockSpec(memory_space=pltpu.VMEM)
    buffers = []
    for sizes, _ in WAVES:
        buffers += wave_buffers(sizes)
    return pl.pallas_call(
        main_kernel,
        name="gradients_and_sum",
        in_specs=[hbm] * 11,
        out_specs=[vm, vm],
        out_shape=[pltpu.VMEM((TOTAL_ROWS, HID), F32), pltpu.VMEM((1, ROWS), F32)],
        scratch_shapes=[
            pltpu.VMEM((FEAT, ROWS), BF16),
            pltpu.VMEM((FEAT, HID), BF16),
            pltpu.VMEM((1, HID), F32),
            pltpu.VMEM((HEADS, HID), BF16),
            pltpu.VMEM((1, HEADS), F32),
            pltpu.VMEM((1, ROWS), jnp.int32),
            pltpu.VMEM((ACT, ATOM, ROWS), F32),
            pltpu.VMEM((1, ROWS), jnp.int32),
            pltpu.VMEM((ATOM, ROWS), jnp.int32),
            pltpu.VMEM((ATOM, ROWS), F32),
            pltpu.VMEM((1, ROWS), F32),
            pltpu.VMEM((HEADS, HID), F32),
            pltpu.VMEM((HEAD, HID), BF16),
            pltpu.VMEM((1088, 128), F32),
            pltpu.VMEM((ATOM, 128), F32),
            pltpu.VMEM((ATOM, 128), F32),
            pltpu.VMEM((SLOT, ROWS), F32),
            pltpu.VMEM((ROWS, HID), BF16),
            pltpu.VMEM((HEAD, ROWS), BF16),
            pltpu.VMEM((ROWS, HID), BF16),
            pltpu.VMEM((1024, 128), F32),
            pltpu.VMEM((TOTAL_ROWS, HID), F32),
            pltpu.SemaphoreType.DMA((15,)),
            pltpu.SemaphoreType.DMA((len(WAVES),)),
            pltpu.SemaphoreType.DMA((len(WAVES), RECEIVES)),
            *buffers,
        ],
        compiler_params=pltpu.CompilerParams(
            vmem_limit_bytes=54 * 1024 * 1024, collective_id=0, has_side_effects=True
        ),
    )(*[in_hbm(x) for x in args])


def finish(tot, ce):
    hbm = pl.BlockSpec(memory_space=pltpu.HBM)
    vm = pl.BlockSpec(memory_space=pltpu.VMEM)
    return pl.pallas_call(
        finish_kernel,
        name="finish",
        in_specs=[vm, vm],
        out_specs=[hbm] * 6,
        out_shape=[
            jax.ShapeDtypeStruct((FEAT, HID), F32),
            jax.ShapeDtypeStruct((1, HID), F32),
            jax.ShapeDtypeStruct((HEADS, HID), F32),
            jax.ShapeDtypeStruct((1, HEADS), F32),
            jax.ShapeDtypeStruct((1, 1), F32),
            jax.ShapeDtypeStruct((1, ROWS), F32),
        ],
        scratch_shapes=[
            pltpu.VMEM((HEADS, HID), F32),
            pltpu.VMEM((1, HID), F32),
            pltpu.VMEM((1, HEADS), F32),
            pltpu.VMEM((1, 1), F32),
            pltpu.VMEM((1, ROWS), F32),
            pltpu.SemaphoreType.DMA((9,)),
        ],
        compiler_params=pltpu.CompilerParams(vmem_limit_bytes=8 * 1024 * 1024),
    )(tot, ce)


def on_device(features, w_one, b_one, w_two, b_two, action, target_probs, next_action, lower_idx, upper_frac, is_weight):
    tot, ce = main(
        features.T, w_one.T, b_one[None, :], w_two.T, b_two[None, :], action[None, :],
        target_probs.transpose(1, 2, 0), next_action[None, :], lower_idx.T, upper_frac.T, is_weight[None, :],
    )
    gw1, gb1, gw2, gb2, loss, prio = finish(tot, ce)
    return gw1.T, gb1[0], gw2.T, gb2[0], loss[0, 0], prio[0]


def solution(mesh):
    in_specs = (
        P("dp", None), P(), P(), P(), P(), P("dp"), P("dp", None, None), P("dp"), P("dp", None), P("dp", None), P("dp"),
    )
    out_specs = (P(), P(), P(), P(), P(), P("dp"))
    return jax.shard_map(on_device, mesh=mesh, in_specs=in_specs, out_specs=out_specs, check_vma=False)
```

```python
import functools

import jax
import jax.numpy as jnp
from jax import lax
from jax.experimental import pallas as pl
from jax.experimental.pallas import tpu as pltpu
from jax.sharding import PartitionSpec as P

MESH = pl.DeviceIdType.MESH
F32, BF16 = jnp.float32, jnp.bfloat16

FEAT, HID, ACT, ATOM, ROWS = 3136, 512, 18, 51, 1024
SLOT = 64
HEAD = ACT * SLOT
HEADS = ACT * ATOM

W1_AT = 928
B1_AT = W1_AT + FEAT
B2_AT = B1_AT + 1
TOP_AT = B2_AT + 2
LOSS_AT = TOP_AT + 1
TOTAL_ROWS = 4096
WAVES = (
    ((128, 128, 128), None),
    ((256, 128, 128), (2, 256)),
    ((256, 256, 256), (2, 384)),
    ((128, 128, 128), (2, 192)),
)
PLAN = "a0A1b0B12c0C1230123012301230132103203213230132"


def main_kernel(
    feat_hbm, w1_hbm, b1_hbm, w2_hbm, b2_hbm, act_hbm, tp_hbm, nact_hbm, low_hbm, frac_hbm, isw_hbm,
    tot, ce_ref,
    feat, w1, b1_ref, w2raw, b2_ref, act_ref, tp, nact_ref, low_ref, frac_ref, isw_ref,
    w2f, w2p, b2col, mlow, mhigh, proj, hid, glt, gp, gb2, part_ref, sems, send_sem, recv_sem, *buffers,
):
    me = lax.axis_index("dp")
    core = me % 2
    sibling = me + 1 - 2 * core
    left, right = slice(0, ROWS // 2), slice(ROWS // 2, ROWS)
    pairs = [(nact_hbm, nact_ref), (low_hbm, low_ref), (frac_hbm, frac_ref)]
    for t in range(4):
        cols = slice(256 * t, 256 * (t + 1))
        pairs.append((tp_hbm.at[:, :, cols], tp.at[:, :, cols]))
    pairs += [
        (w2_hbm, w2raw), (b2_hbm, b2_ref), (b1_hbm, b1_ref), (act_hbm, act_ref), (isw_hbm, isw_ref),
        (w1_hbm, w1), (feat_hbm.at[:, left], feat.at[:, left]), (feat_hbm.at[:, right], feat.at[:, right]),
    ]
    copies = [pltpu.make_async_copy(src, dst, sems.at[i]) for i, (src, dst) in enumerate(pairs)]
    for copy in copies[:7]:
        copy.start()
    near = [sibling]
    for axis in range(3):
        near += ring(me, axis)[1][1:]
    barrier = pltpu.get_barrier_semaphore()
    for device in near:
        pl.semaphore_signal(barrier, inc=1, device_id=(device,), device_id_type=MESH)

    for copy in copies[:4]:
        copy.wait()
    for copy in copies[7:]:
        copy.start()
    atom_row = lax.broadcasted_iota(jnp.int32, (56, 128), 0)
    proj[56:, :] = jnp.zeros((SLOT - 56, ROWS), F32)

    def project(t, carry):
        lanes = pl.ds(pl.multiple_of(t * 128, 128), 128)
        nact = nact_ref[:, lanes]
        probs = jnp.zeros((ATOM, 128), F32)
        for a in range(ACT):
            probs = jnp.where(nact == a, tp[a, :, lanes], probs)
        frac = frac_ref[:, lanes]
        mlow[...] = probs * (1.0 - frac)
        mhigh[...] = probs * frac
        low_sum = jnp.zeros((56, 128), F32)
        high_sum = jnp.zeros((56, 128), F32)
        for j in range(ATOM):
            hot = low_ref[pl.ds(j, 1), lanes] == atom_row
            low_sum = low_sum + jnp.where(hot, mlow[pl.ds(j, 1), :], 0.0)
            high_sum = high_sum + jnp.where(hot, mhigh[pl.ds(j, 1), :], 0.0)
        high_sum = jnp.where(atom_row == 0, 0.0, pltpu.roll(high_sum, 1, 0))
        proj[0:56, lanes] = low_sum + high_sum
        return carry

    lax.fori_loop(0, 2, project, 0)
    for t in range(1, 4):
        copies[3 + t].wait()
        lax.fori_loop(2 * t, 2 * t + 2, project, 0)

    copies[7].wait()
    copies[8].wait()
    w2f[912:, :] = jnp.zeros((24, HID), F32)
    w2f[:HEADS, :] = w2raw[...].astype(F32)
    wrow = lax.broadcasted_iota(jnp.int32, (SLOT, HID), 0)
    for a in range(ACT):
        block = w2f[ATOM * a : ATOM * a + SLOT, :]
        w2p[SLOT * a : SLOT * (a + 1), :] = jnp.where(wrow < ATOM, block, 0.0).astype(BF16)
    b2row = jnp.concatenate([b2_ref[...], jnp.zeros((1, 1024 - HEADS), F32)], axis=1)
    b2col[0:1024, :] = jnp.broadcast_to(b2row, (128, 1024)).T
    b2col[1024:, :] = jnp.zeros((64, 128), F32)

    for copy in copies[9:13]:
        copy.wait()

    for t in range(2):
        copies[13 + t].wait()
        cols = slice(512 * t, 512 * (t + 1))
        pre = lax.dot_general(feat[:, cols], w1[...], (((0,), (0,)), ((), ())), preferred_element_type=F32)
        hid[cols, :] = jnp.maximum(pre + b1_ref[...], 0.0).astype(BF16)

    valid = lax.broadcasted_iota(jnp.int32, (SLOT, 256), 0) < ATOM

    def head(t, carry):
        loss, top = carry
        cols = slice(256 * t, 256 * (t + 1))
        logits = lax.dot_general(w2p[...], hid[cols, :], (((1,), (1,)), ((), ())), preferred_element_type=F32)
        action = act_ref[:, cols]
        chosen = jnp.zeros((SLOT, 256), F32)
        for a in range(ACT):
            bias = b2col[ATOM * a : ATOM * a + SLOT, :]
            biased = logits[SLOT * a : SLOT * (a + 1), :] + jnp.concatenate([bias, bias], axis=1)
            chosen = jnp.where(action == a, biased, chosen)
        chosen = jnp.where(valid, chosen, -1e30)
        shifted = chosen - jnp.max(chosen, axis=0, keepdims=True)
        expd = jnp.where(valid, jnp.exp(shifted), 0.0)
        log_probs = shifted - jnp.log(jnp.sum(expd, axis=0, keepdims=True))
        projected = proj[:, cols]
        cross = -jnp.sum(jnp.where(valid, projected * log_probs, 0.0), axis=0, keepdims=True)
        weight = isw_ref[:, cols]
        probs = jnp.where(valid, jnp.exp(log_probs), 0.0)
        grad = weight * (probs * jnp.sum(projected, axis=0, keepdims=True) - projected)
        grad16 = grad.astype(BF16)
        for a in range(ACT):
            glt[SLOT * a : SLOT * (a + 1), cols] = jnp.where(action == a, grad, 0.0).astype(BF16)
        ce_ref[:, cols] = cross
        return loss + weight * cross, jnp.maximum(top, cross)

    carry = (jnp.zeros((1, 256), F32), jnp.full((1, 256), -jnp.inf, F32))
    for t in range(ROWS // 256):
        carry = head(t, carry)
    loss_row, top_row = carry

    group = 6
    for g in range(ACT // group):
        rows = group * SLOT
        gl = glt[g * rows : (g + 1) * rows, :]
        gw2 = lax.dot_general(gl, hid[...], (((1,), (0,)), ((), ())), preferred_element_type=F32)
        for i in range(group):
            a = g * group + i
            part_ref[ATOM * a : ATOM * (a + 1), :] = gw2[SLOT * i : SLOT * i + ATOM, :]
    part_ref[HEADS:W1_AT, :] = jnp.zeros((W1_AT - HEADS, HID), F32)

    pl.semaphore_wait(barrier, len(near))
    waves, row, at = [], 0, 0
    for i, (sizes, _) in enumerate(WAVES):
        waves.append(Wave(i, sizes, row, me, core, send_sem, recv_sem, part_ref, tot, buffers[6 * i : 6 * (i + 1)]))
        row += 2 * sum(sizes)
    assert row == TOTAL_ROWS
    waves[0].swap()

    def back(t, gb1):
        cols = pl.ds(pl.multiple_of(t * 512, 512), 512)
        gh = lax.dot_general(glt[:, cols], w2p[...], (((0,), (0,)), ((), ())), preferred_element_type=F32)
        g16 = jnp.where(hid[cols, :].astype(F32) > 0.0, gh, 0.0).astype(BF16)
        gp[cols, :] = g16
        return gb1 + jnp.sum(g16.astype(F32), axis=0, keepdims=True)

    gb1 = lax.fori_loop(0, ROWS // 512, back, jnp.zeros((1, HID), F32))

    def grad_w1(wave, half, tiles, size):
        low = wave.row + half * wave.half
        start = jnp.maximum(low - W1_AT, 0)
        span = jnp.minimum(low + wave.half - W1_AT, FEAT) - start

        def tile(i, carry):
            at = start + jnp.minimum(i * size, span - size)
            rows = pl.ds(pl.multiple_of(at, 16), size)
            out = pl.ds(pl.multiple_of(at + W1_AT, 16), size)
            part_ref[out, :] = jnp.dot(feat[rows, :], gp[...], preferred_element_type=F32)
            return carry

        lax.fori_loop(0, tiles, tile, 0)

    def tail_rows():
        for a in range(ACT):
            ga = glt[SLOT * a : SLOT * (a + 1), :].astype(F32)
            gb2[ATOM * a : ATOM * (a + 1), :] = jnp.broadcast_to(jnp.sum(ga, axis=1, keepdims=True), (SLOT, 128))[:ATOM]
        gb2[HEADS:, :] = jnp.zeros((1024 - HEADS, 128), F32)
        gb2_row = gb2[...].T[0:1, :]
        lane = lax.broadcasted_iota(jnp.int32, (1, HID), 1)
        top = jnp.max(top_row)
        loss = jnp.sum(loss_row)
        part_ref[B1_AT:, :] = jnp.concatenate(
            [
                gb1,
                gb2_row[:, :HID],
                gb2_row[:, HID:],
                jnp.where(lane == me, top, 0.0),
                jnp.where(lane == 0, loss, 0.0),
                jnp.zeros((TOTAL_ROWS - LOSS_AT - 1, HID), F32),
            ],
            axis=0,
        )

    steps = [wave.steps() for wave in waves]

    for token in PLAN:
        i = "0ABCD".find(token.upper())
        if i > 0:
            other = token.islower()
            if other and i == len(waves) - 1:
                tail_rows()
            grad_w1(waves[i], 1 - core if other else core, *WAVES[i][1])
            if other:
                waves[i].swap()
        else:
            next(steps[int(token)])
    for wave in waves:
        wave.drain()


def finish_kernel(
    tot, ce, w1_out, b1_out, w2_out, b2_out, loss_out, prio_out, w2_copy, b1_copy, b2_copy, loss_copy, prio_copy, sems,
):
    copies = []

    def copy_out(src, dst):
        copies.append(pltpu.make_async_copy(src, dst, sems.at[len(copies)]))
        copies[-1].start()

    for i in range(4):
        copy_out(tot.at[pl.ds(W1_AT + 784 * i, 784), :], w1_out.at[pl.ds(784 * i, 784), :])
    w2_copy[...] = tot[:HEADS, :]
    copy_out(w2_copy, w2_out)
    b1_copy[...] = tot[B1_AT : B1_AT + 1, :]
    copy_out(b1_copy, b1_out)
    b2_copy[...] = jnp.concatenate([tot[B2_AT : B2_AT + 1, :], tot[B2_AT + 1 : B2_AT + 2, :]], axis=1)[:, :HEADS]
    copy_out(b2_copy, b2_out)
    loss_copy[...] = tot[LOSS_AT : LOSS_AT + 1, 0:1] * (1.0 / (ROWS * 128))
    copy_out(loss_copy, loss_out)
    top = jnp.max(tot[TOP_AT : TOP_AT + 1, 0:128])
    prio_copy[...] = ce[...] / jnp.maximum(top, 1.0)
    copy_out(prio_copy, prio_out)
    for copy in copies:
        copy.wait()


RECEIVES = 16
LO, HI, ALL = slice(0, HID // 2), slice(HID // 2, HID), slice(0, HID)
ORDER = (2, 1, 3, 0)


def rows_at(start, size):
    return pl.ds(pl.multiple_of(start, 8), size)


def lanes_at(p):
    return pl.ds(pl.multiple_of(p * 128, 128), 128)


def ring(me, axis):
    stride = 32 - 33 * axis + 9 * axis * axis
    at = (me // stride) % 4
    return at, [me + stride * ((at + d) % 4 - at) for d in range(4)]


class Wave:
    def __init__(self, index, sizes, row, me, core, send_sem, recv_sem, part, tot, buffers):
        self.row, self.half, self.part, self.tot = row, sum(sizes), part, tot
        self.work, self.plus, self.minus, self.one, self.whole, self.piece = buffers
        self.sizes = sizes
        self.first = [sum(sizes[:s]) for s in range(3)]
        self.base = row + core * self.half
        self.other = row + (1 - core) * self.half
        self.sibling = me + 1 - 2 * core
        self.mine = [[ring(me, (s + k + core) % 3) for k in range(3)] for s in range(3)]
        self.theirs = [ring(me, (s + 1 - core) % 3)[0] for s in range(3)]
        self.send_sem = send_sem.at[index]
        self.recv_sems = [recv_sem.at[index, i] for i in range(RECEIVES)]
        self.sent = 0

    def take(self):
        return self.recv_sems.pop(0)

    def send(self, src, dst, device, recv_sem):
        self.sent += src.shape[0] * src.shape[1]
        pltpu.make_async_remote_copy(
            src_ref=src, dst_ref=dst, send_sem=self.send_sem, recv_sem=recv_sem,
            device_id=(device,), device_id_type=MESH,
        ).start()

    def wait(self, sem, rows, lanes):
        ref = self.part.at[0:rows, 0:lanes]
        pltpu.make_async_copy(ref, ref, sem).wait()

    def drain(self):
        tiles = self.sent // 1024
        self.wait(self.send_sem, tiles // 4 * 8, HID)
        if tiles % 4:
            self.wait(self.send_sem, 8, tiles % 4 * 128)

    def swap(self):
        self.swapped = {d: self.take() for d in ORDER}
        for d in ORDER:
            for s in range(3):
                q = self.sizes[s] // 4
                at = (self.theirs[s] + d) % 4 * q + self.first[s]
                self.send(
                    self.part.at[rows_at(self.other + at, q), :], self.work.at[rows_at(at, q), :], self.sibling,
                    self.swapped[d],
                )

    def scatter(self, blocks, sizes):
        k, send, work, plus, minus, one = 0, self.send, self.work, self.plus, self.minus, self.one
        up, down, rest = self.take(), self.take(), self.take()
        quarter = {}
        for d in ORDER:
            self.wait(self.swapped[d], sum(sizes), HID)
            for s in range(3):
                at, ahead = self.mine[s][k]
                q = sizes[s]
                local = blocks[s] + (at + d) % 4 * q
                rows = rows_at(local, q)
                quarter[s, d] = rows
                work[rows, :] = work[rows, :] + self.part[rows_at(self.base + local, q), :]
                here = pl.ds(0, q)
                if d == 2:
                    send(work.at[rows, LO], one.at[s, here, LO], ahead[1], up)
                    send(work.at[rows, HI], one.at[s, here, HI], ahead[3], down)
                elif d == 1:
                    send(work.at[rows, HI], plus.at[s, here, HI], ahead[1], rest)
                elif d == 3:
                    send(work.at[rows, LO], minus.at[s, here, LO], ahead[3], rest)
        yield
        for name, d, lanes, target, step in ((up, 1, LO, plus, 1), (down, 3, HI, minus, 3)):
            self.wait(name, sum(sizes), HID // 2)
            for s in range(3):
                rows, here = quarter[s, d], pl.ds(0, sizes[s])
                work[rows, lanes] = work[rows, lanes] + one[s, here, lanes]
                send(work.at[rows, lanes], target.at[s, here, lanes], self.mine[s][k][1][step], rest)
        yield
        self.wait(rest, 2 * sum(sizes), HID)
        for s in range(3):
            rows, here = quarter[s, 0], pl.ds(0, sizes[s])
            work[rows, :] = work[rows, :] + (plus[s, here, :] + minus[s, here, :])

    def scatter_straight(self, blocks, sizes):
        whole, work, sem = self.whole, self.work, self.take()
        for d in (2, 1, 3):
            for s in range(3):
                at, ahead = self.mine[s][1]
                rows = rows_at(blocks[s] + (at + d) % 4 * sizes[s], sizes[s])
                self.send(work.at[rows, ALL], whole.at[s, d - 1, pl.ds(0, sizes[s]), :], ahead[d], sem)
        yield
        self.wait(sem, 3 * sum(sizes), HID)
        for s in range(3):
            rows, here = rows_at(blocks[s] + self.mine[s][1][0] * sizes[s], sizes[s]), pl.ds(0, sizes[s])
            work[rows, :] = (work[rows, :] + whole[s, 1, here, :]) + (whole[s, 0, here, :] + whole[s, 2, here, :])

    def put(self, k, blocks, sizes, s, d, lanes, device, sem):
        start = self.base + blocks[s] + (self.mine[s][k][0] + d) % 4 * sizes[s]
        ref = self.tot.at[rows_at(start, sizes[s]), lanes]
        self.send(ref, ref, device, sem)

    def gather_straight(self, blocks, sizes):
        sem = self.take()
        for d in (2, 1, 3):
            for s in range(3):
                self.put(1, blocks, sizes, s, 0, ALL, self.mine[s][1][1][d], sem)
        yield
        self.wait(sem, 3 * sum(sizes), HID)

    def gather(self, blocks, sizes):
        up, down, rest, far, both = self.take(), self.take(), self.take(), self.take(), self.take()
        put = functools.partial(self.put, 0, blocks, sizes)

        def to_sibling(*quarters):
            for s in range(3):
                for d in quarters:
                    put(s, d, ALL, self.sibling, both)

        for lanes, step, sem in ((LO, 1, up), (HI, 3, down), (HI, 1, rest), (LO, 3, rest)):
            for s in range(3):
                put(s, 0, lanes, self.mine[s][0][1][step], sem)
        to_sibling(0)
        yield
        for sem, d, lanes, step in ((up, 3, LO, 1), (down, 1, HI, 3)):
            self.wait(sem, sum(sizes), HID // 2)
            for s in range(3):
                put(s, d, lanes, self.mine[s][0][1][step], far)
        yield
        self.wait(rest, sum(sizes), HID)
        to_sibling(3, 1)
        self.wait(far, sum(sizes), HID)
        to_sibling(2)
        yield
        self.wait(both, self.half, HID)

    def steps(self):
        size_a = [size // 4 for size in self.sizes]
        size_b = [size // 16 for size in self.sizes]
        block_a = self.first
        yield from self.scatter(block_a, size_a)
        block_b = [block_a[s] + self.mine[s][0][0] * size_a[s] for s in range(3)]
        yield from self.scatter_straight(block_b, size_b)
        block_c = [block_b[s] + self.mine[s][1][0] * size_b[s] for s in range(3)]

        piece, work, tot = self.piece, self.work, self.tot
        last, final = self.take(), self.take()
        for d in (2, 1, 3):
            for s in range(3):
                at, ahead = self.mine[s][2]
                self.send(
                    work.at[rows_at(block_c[s], size_b[s]), lanes_at((at + d) % 4)],
                    piece.at[s, d - 1, pl.ds(0, size_b[s]), :], ahead[d], last,
                )
        yield
        self.wait(last, 3 * sum(size_b), 128)
        for s in range(3):
            at, ahead = self.mine[s][2]
            here = pl.ds(0, size_b[s])
            got = work[rows_at(block_c[s], size_b[s]), lanes_at(at)] + (piece[s, 0, here, :] + piece[s, 2, here, :])
            rows = rows_at(self.base + block_c[s], size_b[s])
            tot[rows, lanes_at(at)] = got + piece[s, 1, here, :]
            for d in (2, 1, 3):
                ref = tot.at[rows, lanes_at(at)]
                self.send(ref, ref, ahead[d], final)
        yield
        self.wait(final, 3 * sum(size_b), 128)
        yield from self.gather_straight(block_b, size_b)
        yield from self.gather(block_a, size_a)
        yield


def wave_buffers(sizes):
    q, half = max(sizes) // 4, sum(sizes)
    return [
        pltpu.VMEM((half, HID), F32),
        pltpu.VMEM((3, q, HID), F32),
        pltpu.VMEM((3, q, HID), F32),
        pltpu.VMEM((3, q, HID), F32),
        pltpu.VMEM((3, 3, q // 4, HID), F32),
        pltpu.VMEM((3, 3, q // 4, 128), F32),
    ]


def in_hbm(x):
    return pltpu.with_memory_space_constraint(x, pltpu.HBM)


def main(*args):
    hbm = pl.BlockSpec(memory_space=pltpu.HBM)
    vm = pl.BlockSpec(memory_space=pltpu.VMEM)
    buffers = []
    for sizes, _ in WAVES:
        buffers += wave_buffers(sizes)
    return pl.pallas_call(
        main_kernel,
        name="gradients_and_sum",
        in_specs=[hbm] * 11,
        out_specs=[vm, vm],
        out_shape=[pltpu.VMEM((TOTAL_ROWS, HID), F32), pltpu.VMEM((1, ROWS), F32)],
        scratch_shapes=[
            pltpu.VMEM((FEAT, ROWS), BF16),
            pltpu.VMEM((FEAT, HID), BF16),
            pltpu.VMEM((1, HID), F32),
            pltpu.VMEM((HEADS, HID), BF16),
            pltpu.VMEM((1, HEADS), F32),
            pltpu.VMEM((1, ROWS), jnp.int32),
            pltpu.VMEM((ACT, ATOM, ROWS), F32),
            pltpu.VMEM((1, ROWS), jnp.int32),
            pltpu.VMEM((ATOM, ROWS), jnp.int32),
            pltpu.VMEM((ATOM, ROWS), F32),
            pltpu.VMEM((1, ROWS), F32),
            pltpu.VMEM((936, HID), F32),
            pltpu.VMEM((HEAD, HID), BF16),
            pltpu.VMEM((1088, 128), F32),
            pltpu.VMEM((ATOM, 128), F32),
            pltpu.VMEM((ATOM, 128), F32),
            pltpu.VMEM((SLOT, ROWS), F32),
            pltpu.VMEM((ROWS, HID), BF16),
            pltpu.VMEM((HEAD, ROWS), BF16),
            pltpu.VMEM((ROWS, HID), BF16),
            pltpu.VMEM((1024, 128), F32),
            pltpu.VMEM((TOTAL_ROWS, HID), F32),
            pltpu.SemaphoreType.DMA((15,)),
            pltpu.SemaphoreType.DMA((len(WAVES),)),
            pltpu.SemaphoreType.DMA((len(WAVES), RECEIVES)),
            *buffers,
        ],
        compiler_params=pltpu.CompilerParams(
            vmem_limit_bytes=54 * 1024 * 1024, collective_id=0, has_side_effects=True
        ),
    )(*[in_hbm(x) for x in args])


def finish(tot, ce):
    hbm = pl.BlockSpec(memory_space=pltpu.HBM)
    vm = pl.BlockSpec(memory_space=pltpu.VMEM)
    return pl.pallas_call(
        finish_kernel,
        name="finish",
        in_specs=[vm, vm],
        out_specs=[hbm] * 6,
        out_shape=[
            jax.ShapeDtypeStruct((FEAT, HID), F32),
            jax.ShapeDtypeStruct((1, HID), F32),
            jax.ShapeDtypeStruct((HEADS, HID), F32),
            jax.ShapeDtypeStruct((1, HEADS), F32),
            jax.ShapeDtypeStruct((1, 1), F32),
            jax.ShapeDtypeStruct((1, ROWS), F32),
        ],
        scratch_shapes=[
            pltpu.VMEM((HEADS, HID), F32),
            pltpu.VMEM((1, HID), F32),
            pltpu.VMEM((1, HEADS), F32),
            pltpu.VMEM((1, 1), F32),
            pltpu.VMEM((1, ROWS), F32),
            pltpu.SemaphoreType.DMA((9,)),
        ],
        compiler_params=pltpu.CompilerParams(vmem_limit_bytes=8 * 1024 * 1024),
    )(tot, ce)


def on_device(features, w_one, b_one, w_two, b_two, action, target_probs, next_action, lower_idx, upper_frac, is_weight):
    tot, ce = main(
        features.T, w_one.T, b_one[None, :], w_two.T, b_two[None, :], action[None, :],
        target_probs.transpose(1, 2, 0), next_action[None, :], lower_idx.T, upper_frac.T, is_weight[None, :],
    )
    gw1, gb1, gw2, gb2, loss, prio = finish(tot, ce)
    return gw1.T, gb1[0], gw2.T, gb2[0], loss[0, 0], prio[0]


def solution(mesh):
    in_specs = (
        P("dp", None), P(), P(), P(), P(), P("dp"), P("dp", None, None), P("dp"), P("dp", None), P("dp", None), P("dp"),
    )
    out_specs = (P(), P(), P(), P(), P(), P("dp"))
    return jax.shard_map(on_device, mesh=mesh, in_specs=in_specs, out_specs=out_specs, check_vma=False)
```
